8 devices in a mesh: dp: 4 (over z, y, x), emb: 2 (over core).
Axes of the slice: x: 2, y: 2, z: 1, core: 2. Of those that a mesh axis runs over, the one named last changes fastest.
Arguments:
- tok_ids: int32 [8192], P(('dp', 'emb'))
- resid_in: bfloat16 [8192, 896], P(('dp', 'emb'))
- cot_out: bfloat16 [8192, 896], P(('dp', 'emb'))
- tables: bfloat16 [6, 151936, 128], P(None, 'emb')
- w_up: bfloat16 [6, 896, 4864], replicated
- w_down: bfloat16 [6, 4864, 896], replicated
- w_gate: bfloat16 [6, 896, 128], replicated
- w_proj: bfloat16 [6, 128, 896], replicated
Outputs:
- output 1: bfloat16 [8192, 896], P(('dp', 'emb'))
- output 2: float32 [6, 151936, 128], P(None, 'emb')
All inputs are finite; a program needn't handle non-finite values.
Results may differ from the reference program's by a relative error of at most 0.0149798.
Values are sent between devices in bfloat16 or wider.
A program may use at most 1.75 GiB of HBM per device.

```python
import jax
import jax.numpy as jnp
from jax import lax

TOKENS_DEV = 1024
LAYERS = 6
D_MODEL = 896
FFN_DIM = 4864
EMB_DIM = 128
VOCAB_SIZE = 151936
NUM_DP = 4
NUM_EMB = 2
CAP_ROWS = 768

N_TOKENS = TOKENS_DEV * NUM_DP * NUM_EMB
RANGE_ROWS = VOCAB_SIZE // NUM_EMB
HOT_SET = min(16, RANGE_ROWS)
NORM_EPS = 1e-6


def draw_ids(id_key):
    key_list = jax.random.split(id_key, 9)
    n_dev = NUM_DP * NUM_EMB
    draw_shape = (n_dev, TOKENS_DEV)
    tok_pos = jnp.arange(TOKENS_DEV, dtype=jnp.int32)[None, :]
    hot_top = jax.random.randint(key_list[0], (n_dev, 1), 1, NUM_EMB + 1)
    hot_owner = jax.random.randint(key_list[1], (n_dev, 1), 0, hot_top)
    shift_by = jax.random.randint(key_list[2], (n_dev, 1), 0, NUM_EMB - 1)
    spread = (hot_owner + 1 + (tok_pos - CAP_ROWS + shift_by) % (NUM_EMB - 1)) % NUM_EMB
    owner_seq = jnp.where(tok_pos < CAP_ROWS, hot_owner, spread)
    scores = jax.random.randint(key_list[3], draw_shape, 0, TOKENS_DEV) * TOKENS_DEV + tok_pos
    perm_order = jnp.argsort(scores, axis=1)
    owner_ids = jnp.take_along_axis(owner_seq, perm_order, axis=1)
    is_hot = jax.random.randint(key_list[4], draw_shape, 0, 4) == 0
    hot_off = jax.random.randint(key_list[5], draw_shape, 0, HOT_SET)
    span_a = jax.random.randint(key_list[6], draw_shape, 1, RANGE_ROWS + 1)
    span_b = jax.random.randint(key_list[7], draw_shape, 1, span_a + 1)
    tail_off = jax.random.randint(key_list[8], draw_shape, 0, span_b)
    offset = jnp.where(is_hot, hot_off, tail_off)
    return (owner_ids * RANGE_ROWS + offset).reshape(-1).astype(jnp.int32)


def setup_inputs(seed: int = 0) -> dict:
    root_key = jax.random.key(seed)
    key_list = jax.random.split(root_key, 8)
    tok_ids = draw_ids(key_list[0])
    resid_in = jax.random.normal(key_list[1], (N_TOKENS, D_MODEL), jnp.float32).astype(jnp.bfloat16)
    cot_out = jax.random.normal(key_list[2], (N_TOKENS, D_MODEL), jnp.float32).astype(jnp.bfloat16)
    tables = (0.5 * jax.random.normal(key_list[3], (LAYERS, VOCAB_SIZE, EMB_DIM), jnp.float32)).astype(jnp.bfloat16)
    w_up = (jax.random.normal(key_list[4], (LAYERS, D_MODEL, FFN_DIM), jnp.float32) * D_MODEL ** -0.5).astype(jnp.bfloat16)
    w_down = (jax.random.normal(key_list[5], (LAYERS, FFN_DIM, D_MODEL), jnp.float32) * (0.5 * FFN_DIM ** -0.5)).astype(jnp.bfloat16)
    w_gate = (jax.random.normal(key_list[6], (LAYERS, D_MODEL, EMB_DIM), jnp.float32) * D_MODEL ** -0.5).astype(jnp.bfloat16)
    w_proj = (jax.random.normal(key_list[7], (LAYERS, EMB_DIM, D_MODEL), jnp.float32) * EMB_DIM ** -0.5).astype(jnp.bfloat16)
    return {'tok_ids': tok_ids, 'resid_in': resid_in, 'cot_out': cot_out, 'tables': tables, 'w_up': w_up, 'w_down': w_down, 'w_gate': w_gate, 'w_proj': w_proj}


def rms_norm(x_f32):
    return x_f32 * lax.rsqrt(jnp.mean(x_f32 * x_f32, axis=-1, keepdims=True) + NORM_EPS)


def layer_forward(resid_cur, fetched, w_up_l, w_down_l, w_gate_l, w_proj_l):
    x_f32 = resid_cur.astype(jnp.float32)
    normed = rms_norm(x_f32).astype(jnp.bfloat16)
    hidden = jax.nn.gelu(jnp.dot(normed, w_up_l, preferred_element_type=jnp.float32)).astype(jnp.bfloat16)
    mlp_out = jnp.dot(hidden, w_down_l, preferred_element_type=jnp.float32)
    gate_act = jax.nn.gelu(jnp.dot(normed, w_gate_l, preferred_element_type=jnp.float32))
    mixed_in = (gate_act * fetched).astype(jnp.bfloat16)
    proj_out = jnp.dot(mixed_in, w_proj_l, preferred_element_type=jnp.float32)
    return (x_f32 + mlp_out + proj_out).astype(jnp.bfloat16)


def reference(tok_ids, resid_in, cot_out, tables, w_up, w_down, w_gate, w_proj):
    def fwd_step(resid_cur, layer_params):
        table_l, w_up_l, w_down_l, w_gate_l, w_proj_l = layer_params
        fetched = jnp.take(table_l, tok_ids, axis=0).astype(jnp.float32)
        resid_next = layer_forward(resid_cur, fetched, w_up_l, w_down_l, w_gate_l, w_proj_l)
        return resid_next, resid_cur

    resid_out, resid_saved = lax.scan(fwd_step, resid_in, (tables, w_up, w_down, w_gate, w_proj))

    def bwd_step(cot_next, layer_params):
        resid_cur, table_l, w_up_l, w_down_l, w_gate_l, w_proj_l = layer_params
        fetched = jnp.take(table_l, tok_ids, axis=0).astype(jnp.float32)

        def local_layer(resid_arg, fetched_arg):
            return layer_forward(resid_arg, fetched_arg, w_up_l, w_down_l, w_gate_l, w_proj_l)

        pullback = jax.vjp(local_layer, resid_cur, fetched)[1]
        cot_cur, d_fetched = pullback(cot_next)
        d_table = jax.ops.segment_sum(d_fetched, tok_ids, num_segments=VOCAB_SIZE)
        return cot_cur, d_table

    cot_first, d_tables = lax.scan(bwd_step, cot_out, (resid_saved, tables, w_up, w_down, w_gate, w_proj), reverse=True)
    return resid_out, d_tables
```

```python
import functools

import jax
import jax.numpy as jnp
from jax import lax
from jax.experimental import pallas as pl
from jax.experimental.pallas import tpu as pltpu
from jax.sharding import PartitionSpec as P

NORM_EPS = 1e-6
GELU_K = 0.7978845608028654
GELU_A = 0.044715
F_TILE = 256
ROW_CHUNK = 256
OUT_ROWS = 1024
PLACE_UNROLL = 4
FETCH_TOK = 128
F32 = jnp.float32
BF16 = jnp.bfloat16


def gelu_pair(x):
    sq = x * x
    t = jnp.tanh(x * (GELU_K + (GELU_K * GELU_A) * sq))
    cdf = 0.5 + 0.5 * t
    slope = cdf + (0.5 * x) * (1.0 - t * t) * (GELU_K + (3.0 * GELU_K * GELU_A) * sq)
    return x * cdf, slope


def dot_nn(a, b):
    return lax.dot_general(a, b, (((1,), (0,)), ((), ())), preferred_element_type=F32)


def dot_nt(a, b):
    return lax.dot_general(a, b, (((1,), (1,)), ((), ())), preferred_element_type=F32)


def row_chunks(rows):
    return [pl.ds(r, ROW_CHUNK) for r in range(0, rows, ROW_CHUNK)]


def forward_body(n_layers, n_tiles, x_ref, e_ref, wu_ref, wd_ref, wg_ref, wp_ref, out_ref, xs_ref, dg_ref, gp_ref, x_s, u_s, acc_s):
    layer, tile = pl.program_id(0), pl.program_id(1)
    chunks = row_chunks(x_s.shape[0])

    @pl.when((layer == 0) & (tile == 0))
    def _():
        x_s[...] = x_ref[...]

    @pl.when(tile == 0)
    def _():
        for r in chunks:
            x_bf = x_s[r, :]
            xs_ref[0, r, :] = x_bf
            x_f = x_bf.astype(F32)
            u = (x_f * lax.rsqrt(jnp.mean(x_f * x_f, axis=-1, keepdims=True) + NORM_EPS)).astype(BF16)
            u_s[r, :] = u
            gate_pre = dot_nn(u, wg_ref[0])
            gp_ref[0, r, :] = gate_pre
            gate_act, _ = gelu_pair(gate_pre)
            mixed = (gate_act * e_ref[0, r, :].astype(F32)).astype(BF16)
            acc_s[r, :] = x_f + dot_nn(mixed, wp_ref[0])

    for r in chunks:
        up = dot_nn(u_s[r, :], wu_ref[0])
        act, slope = gelu_pair(up)
        dg_ref[0, 0, r, :] = slope
        acc_s[r, :] += dot_nn(act.astype(BF16), wd_ref[0])

    @pl.when(tile == n_tiles - 1)
    def _():
        x_s[...] = acc_s[...].astype(BF16)

    @pl.when((tile == n_tiles - 1) & (layer == n_layers - 1))
    def _():
        out_ref[...] = x_s[...]


def run_forward(resid_in, fetched, w_up, w_down, w_gate, w_proj):
    n_layers, d_model, ffn = w_up.shape
    rows, e_dim = resid_in.shape[0], w_gate.shape[2]
    n_tiles = ffn // F_TILE
    whole = pl.BlockSpec((rows, d_model), lambda l, j: (0, 0))
    per_layer = lambda *s: pl.BlockSpec((1,) + s, lambda l, j: (l, 0, 0))
    return pl.pallas_call(
        functools.partial(forward_body, n_layers, n_tiles),
        grid=(n_layers, n_tiles),
        in_specs=[
            whole,
            per_layer(rows, e_dim),
            pl.BlockSpec((1, d_model, F_TILE), lambda l, j: (l, 0, j)),
            pl.BlockSpec((1, F_TILE, d_model), lambda l, j: (l, j, 0)),
            per_layer(d_model, e_dim),
            per_layer(e_dim, d_model),
        ],
        out_specs=[
            whole,
            per_layer(rows, d_model),
            pl.BlockSpec((1, 1, rows, F_TILE), lambda l, j: (l, j, 0, 0)),
            per_layer(rows, e_dim),
        ],
        out_shape=[
            jax.ShapeDtypeStruct((rows, d_model), BF16),
            jax.ShapeDtypeStruct((n_layers, rows, d_model), BF16),
            jax.ShapeDtypeStruct((n_layers, n_tiles, rows, F_TILE), F32),
            jax.ShapeDtypeStruct((n_layers, rows, e_dim), F32),
        ],
        scratch_shapes=[pltpu.VMEM((rows, d_model), BF16), pltpu.VMEM((rows, d_model), BF16), pltpu.VMEM((rows, d_model), F32)],
        cost_estimate=pl.CostEstimate(flops=4 * n_layers * rows * d_model * ffn, bytes_accessed=n_layers * 40_000_000, transcendentals=0),
        compiler_params=pltpu.CompilerParams(dimension_semantics=('arbitrary', 'arbitrary'), vmem_limit_bytes=56 * 2**20),
        name='forward',
    )(resid_in, fetched, w_up, w_down, w_gate, w_proj)


def backward_body(n_tiles, c_ref, xs_ref, e_ref, gp_ref, dg_ref, wu_ref, wd_ref, wg_ref, wp_ref, cot_ref, gr_ref, dng_s, acc_s):
    tile = pl.program_id(0)
    chunks = row_chunks(c_ref.shape[0])

    @pl.when(tile == 0)
    def _():
        for r in chunks:
            d_mixed = dot_nt(c_ref[r, :], wp_ref[0]).astype(BF16).astype(F32)
            gate_act, slope = gelu_pair(gp_ref[0, r, :])
            gr_ref[r, :] = gate_act * d_mixed
            d_gate = (slope * (d_mixed * e_ref[0, r, :].astype(F32))).astype(BF16)
            dng_s[r, :] = dot_nt(d_gate, wg_ref[0]).astype(BF16)
            acc_s[r, :] = jnp.zeros((ROW_CHUNK, acc_s.shape[1]), F32)

    for r in chunks:
        d_hidden = dot_nt(c_ref[r, :], wd_ref[0]).astype(BF16).astype(F32)
        d_up = (d_hidden * dg_ref[0, 0, r, :]).astype(BF16)
        acc_s[r, :] += dot_nt(d_up, wu_ref[0])

    @pl.when(tile == n_tiles - 1)
    def _():
        for r in chunks:
            d_n = (acc_s[r, :].astype(BF16).astype(F32) + dng_s[r, :].astype(F32)).astype(BF16).astype(F32)
            x_f = xs_ref[0, r, :].astype(F32)
            inv = lax.rsqrt(jnp.mean(x_f * x_f, axis=-1, keepdims=True) + NORM_EPS)
            proj = jnp.mean(d_n * x_f, axis=-1, keepdims=True)
            d_x = d_n * inv - x_f * (inv * inv * inv * proj)
            cot_ref[r, :] = (c_ref[r, :].astype(F32) + d_x).astype(BF16)


def run_backward(layer, cot, xs, fetched, gp, dg, w_up, w_down, w_gate, w_proj):
    _, d_model, ffn = w_up.shape
    rows, e_dim = cot.shape[0], w_gate.shape[2]
    n_tiles = ffn // F_TILE
    whole = lambda *s: pl.BlockSpec(s, lambda j: (0, 0))
    at_layer = lambda *s: pl.BlockSpec((1,) + s, lambda j: (layer, 0, 0))
    return pl.pallas_call(
        functools.partial(backward_body, n_tiles),
        grid=(n_tiles,),
        in_specs=[
            whole(rows, d_model),
            at_layer(rows, d_model),
            at_layer(rows, e_dim),
            at_layer(rows, e_dim),
            pl.BlockSpec((1, 1, rows, F_TILE), lambda j: (layer, j, 0, 0)),
            pl.BlockSpec((1, d_model, F_TILE), lambda j: (layer, 0, j)),
            pl.BlockSpec((1, F_TILE, d_model), lambda j: (layer, j, 0)),
            at_layer(d_model, e_dim),
            at_layer(e_dim, d_model),
        ],
        out_specs=[whole(rows, d_model), whole(rows, e_dim)],
        out_shape=[jax.ShapeDtypeStruct((rows, d_model), BF16), jax.ShapeDtypeStruct((rows, e_dim), F32)],
        scratch_shapes=[pltpu.VMEM((rows, d_model), BF16), pltpu.VMEM((rows, d_model), F32)],
        cost_estimate=pl.CostEstimate(flops=4 * rows * d_model * ffn, bytes_accessed=40_000_000, transcendentals=0),
        compiler_params=pltpu.CompilerParams(dimension_semantics=('arbitrary',), vmem_limit_bytes=56 * 2**20),
        name='backward',
    )(cot, xs, fetched, gp, dg, w_up, w_down, w_gate, w_proj)


def fetch_body(n_layers, n_tok, n_steps, off_ref, table_ref, out_ref, buf, sems):
    step = pl.program_id(0)

    def issue(at, slot):
        def go(i, carry):
            for k in range(8):
                tok = i * 8 + k
                tile = off_ref[at * n_tok + tok] // 8
                pltpu.make_async_copy(table_ref.at[:, pl.ds(pl.multiple_of(tile * 8, 8), 8), :], buf.at[slot, tok], sems.at[slot]).start()
            return carry

        lax.fori_loop(0, n_tok // 8, go, 0)

    @pl.when(step == 0)
    def _():
        issue(0, 0)

    @pl.when(step + 1 < n_steps)
    def _():
        issue(step + 1, (step + 1) % 2)

    slot = step % 2
    pltpu.make_async_copy(buf.at[slot], buf.at[slot], sems.at[slot]).wait()
    sub = lax.broadcasted_iota(jnp.int32, (8, 128), 0)

    def pick(i, carry):
        halves = [[None, None] for _ in range(n_layers)]
        for half in range(2):
            for k in range(8):
                tok = i * 16 + half * 8 + k
                shift = (k + 8 - off_ref[step * n_tok + tok] % 8) % 8
                for l in range(n_layers):
                    moved = pltpu.roll(buf[slot, tok, l].astype(F32), shift, axis=0)
                    halves[l][half] = moved if k == 0 else jnp.where(sub == k, moved, halves[l][half])
        for l in range(n_layers):
            out_ref[l, pl.ds(pl.multiple_of(i * 16, 16), 16), :] = jnp.concatenate(halves[l], axis=0).astype(BF16)
        return carry

    lax.fori_loop(0, n_tok // 16, pick, 0)


def run_fetch(tables, offsets):
    n_layers, _, e_dim = tables.shape
    n_rows = offsets.shape[0]
    n_steps = n_rows // FETCH_TOK
    return pl.pallas_call(
        functools.partial(fetch_body, n_layers, FETCH_TOK, n_steps),
        grid_spec=pltpu.PrefetchScalarGridSpec(
            num_scalar_prefetch=1,
            grid=(n_steps,),
            in_specs=[pl.BlockSpec(memory_space=pl.ANY)],
            out_specs=pl.BlockSpec((n_layers, FETCH_TOK, e_dim), lambda i, off: (0, i, 0)),
            scratch_shapes=[pltpu.VMEM((2, FETCH_TOK, n_layers, 8, e_dim), BF16), pltpu.SemaphoreType.DMA((2,))],
        ),
        out_shape=jax.ShapeDtypeStruct((n_layers, n_rows, e_dim), BF16),
        cost_estimate=pl.CostEstimate(flops=2_000_000_000, bytes_accessed=30_000_000, transcendentals=0),
        compiler_params=pltpu.CompilerParams(dimension_semantics=('arbitrary',)),
        name='fetch_rows',
    )(offsets, tables)


def place_body(n_group, idx_bits, starts_ref, keys_ref, *refs):
    rows_refs, out_ref = refs[:n_group], refs[-1]
    block = pl.program_id(0)
    out_ref[...] = jnp.zeros_like(out_ref)
    start, end = starts_ref[block], starts_ref[block + 1]
    base = block * OUT_ROWS

    def go(i, carry):
        prev, accs = carry[0], list(carry[1:])
        for u in range(PLACE_UNROLL):
            k = start + i * PLACE_UNROLL + u
            key = keys_ref[jnp.minimum(k, end - 1)]
            src = key & ((1 << idx_bits) - 1)
            row_id = key >> idx_bits
            fresh, live = row_id != prev, k < end
            for g in range(n_group):
                row = jnp.where(live, rows_refs[g][pl.ds(src, 1), :], 0.0)
                accs[g] = row + jnp.where(fresh, 0.0, accs[g])
                out_ref[g, pl.ds(row_id - base, 1), :] = accs[g]
            prev = row_id
        return (prev, *accs)

    zero = jnp.zeros((1, out_ref.shape[2]), F32)
    lax.fori_loop(0, (end - start + PLACE_UNROLL - 1) // PLACE_UNROLL, go, (jnp.int32(-1),) + (zero,) * n_group)


def run_place(group, starts, keys, rows_list, d_tables, shape):
    n_group = len(rows_list)
    n_rows, e_dim = rows_list[0].shape
    idx_bits = (n_rows - 1).bit_length()
    args = [starts, keys, *rows_list]
    in_specs = [pl.BlockSpec((n_rows, e_dim), lambda i, s, k: (0, 0)) for _ in rows_list]
    aliases = {}
    if d_tables is not None:
        aliases = {len(args): 0}
        args.append(d_tables)
        in_specs.append(pl.BlockSpec(memory_space=pl.ANY))
    return pl.pallas_call(
        functools.partial(place_body, n_group, idx_bits),
        grid_spec=pltpu.PrefetchScalarGridSpec(
            num_scalar_prefetch=2,
            grid=(pl.cdiv(shape[1], OUT_ROWS),),
            in_specs=in_specs,
            out_specs=pl.BlockSpec((n_group, OUT_ROWS, e_dim), lambda i, s, k: (group, i, 0)),
        ),
        out_shape=jax.ShapeDtypeStruct(shape, F32),
        input_output_aliases=aliases,
        cost_estimate=pl.CostEstimate(flops=30_000_000_000, bytes_accessed=n_group * 44_000_000, transcendentals=0),
        compiler_params=pltpu.CompilerParams(dimension_semantics=('arbitrary',), vmem_limit_bytes=48 * 2**20),
        name='place_rows',
    )(*args)


def solution(mesh):
    n_emb = mesh.shape['emb']
    tok_spec = P(('dp', 'emb'))
    act_spec = P(('dp', 'emb'), None)
    table_spec = P(None, 'emb', None)
    full_spec = P(None, None, None)
    swap = [(i, (i + 1) % n_emb) for i in range(n_emb)]

    def device_body(tok_ids, resid_in, cot_out, tables, w_up, w_down, w_gate, w_proj):
        n_layers, range_rows, e_dim = tables.shape
        tok_count = tok_ids.shape[0]
        base = lax.axis_index('emb') * range_rows

        own_off = tok_ids - base
        own_mask = (own_off >= 0) & (own_off < range_rows)
        peer_ids = lax.ppermute(tok_ids, 'emb', swap)
        offsets = jnp.clip(jnp.concatenate([own_off, peer_ids - base]), 0, range_rows - 1)
        served = run_fetch(tables, offsets)
        from_peer = lax.ppermute(served[:, tok_count:], 'emb', swap)
        fetched = jnp.where(own_mask[None, :, None], served[:, :tok_count], from_peer)

        all_ids = lax.all_gather(tok_ids, ('dp', 'emb'), axis=0, tiled=True)
        n_all = all_ids.shape[0]
        idx_bits = (n_all - 1).bit_length()
        all_off = all_ids - base
        all_off = jnp.where((all_off >= 0) & (all_off < range_rows), all_off, range_rows)
        keys = jnp.sort((all_off << idx_bits) | jnp.arange(n_all, dtype=jnp.int32))
        n_blocks = pl.cdiv(range_rows, OUT_ROWS)
        bounds = jnp.minimum(jnp.arange(n_blocks + 1, dtype=jnp.int32) * OUT_ROWS, range_rows)
        starts = jnp.sum((all_off[None, :] < bounds[:, None]).astype(jnp.int32), axis=1)

        resid_out, xs, dg, gp = run_forward(resid_in, fetched, w_up, w_down, w_gate, w_proj)

        cot = cot_out
        rows_list = [None] * n_layers
        for layer in reversed(range(n_layers)):
            cot, grad_rows = run_backward(layer, cot, xs, fetched, gp, dg, w_up, w_down, w_gate, w_proj)
            rows_list[layer] = lax.all_gather(grad_rows, ('dp', 'emb'), axis=0, tiled=True)

        d_tables = None
        per_group = n_layers // 2
        for group in (1, 0):
            d_tables = run_place(group, starts, keys, rows_list[group * per_group:(group + 1) * per_group], d_tables, tables.shape)
        return resid_out, d_tables

    return jax.shard_map(device_body, mesh=mesh, in_specs=(tok_spec, act_spec, act_spec, table_spec, full_spec, full_spec, full_spec, full_spec), out_specs=(act_spec, table_spec), check_vma=False)
```

```python
import functools

import jax
import jax.numpy as jnp
from jax import lax
from jax.experimental import pallas as pl
from jax.experimental.pallas import tpu as pltpu
from jax.sharding import PartitionSpec as P

NORM_EPS = 1e-6
GELU_K = 0.7978845608028654
GELU_A = 0.044715
F_TILE = 256
FWD_CHUNK = 256
BWD_CHUNK = 1024
OUT_ROWS = 1024
PLACE_UNROLL = 8
PLACE_BUFS = 4
FETCH_TOK = 128
F32 = jnp.float32
BF16 = jnp.bfloat16


def gelu_pair(x):
    sq = x * x
    t = jnp.tanh(x * (GELU_K + (GELU_K * GELU_A) * sq))
    cdf = 0.5 + 0.5 * t
    slope = cdf + (0.5 * x) * (1.0 - t * t) * (GELU_K + (3.0 * GELU_K * GELU_A) * sq)
    return x * cdf, slope


def dot_nn(a, b):
    return lax.dot_general(a, b, (((1,), (0,)), ((), ())), preferred_element_type=F32)


def dot_nt(a, b):
    return lax.dot_general(a, b, (((1,), (1,)), ((), ())), preferred_element_type=F32)


def row_chunks(rows, size):
    return [pl.ds(r, min(size, rows)) for r in range(0, rows, size)]


def forward_body(n_layers, n_tiles, x_ref, e_ref, wu_ref, wd_ref, wg_ref, wp_ref, out_ref, xs_ref, dg_ref, gp_ref, x_s, u_s, h_s, acc_s):
    layer, tile = pl.program_id(0), pl.program_id(1)
    chunks = row_chunks(x_s.shape[0], FWD_CHUNK)

    def up_half(r):
        act, slope = gelu_pair(dot_nn(u_s[r, :], wu_ref[0]))
        dg_ref[0, 0, r, :] = slope
        h_s[r, :] = act.astype(BF16)

    def down_half(r):
        acc_s[r, :] += dot_nn(h_s[r, :], wd_ref[0])

    @pl.when((layer == 0) & (tile == 0))
    def _():
        x_s[...] = x_ref[...]

    @pl.when(tile == 0)
    def _():
        for r in chunks:
            x_bf = x_s[r, :]
            xs_ref[0, r, :] = x_bf
            x_f = x_bf.astype(F32)
            u = (x_f * lax.rsqrt(jnp.mean(x_f * x_f, axis=-1, keepdims=True) + NORM_EPS)).astype(BF16)
            u_s[r, :] = u
            gate_pre = dot_nn(u, wg_ref[0])
            gp_ref[0, r, :] = gate_pre
            gate_act, _ = gelu_pair(gate_pre)
            mixed = (gate_act * e_ref[0, r, :].astype(F32)).astype(BF16)
            acc_s[r, :] = x_f + dot_nn(mixed, wp_ref[0])
            up_half(r)

    @pl.when((tile > 0) & (tile < n_tiles))
    def _():
        for r in chunks:
            down_half(r)
            up_half(r)

    @pl.when(tile == n_tiles)
    def _():
        for r in chunks:
            x_s[r, :] = (acc_s[r, :] + dot_nn(h_s[r, :], wd_ref[0])).astype(BF16)

    @pl.when((tile == n_tiles) & (layer == n_layers - 1))
    def _():
        out_ref[...] = x_s[...]


def run_forward(resid_in, fetched, w_up, w_down, w_gate, w_proj):
    n_layers, d_model, ffn = w_up.shape
    rows, e_dim = resid_in.shape[0], w_gate.shape[2]
    n_tiles = ffn // F_TILE
    whole = pl.BlockSpec((rows, d_model), lambda l, j: (0, 0))
    per_layer = lambda *s: pl.BlockSpec((1,) + s, lambda l, j: (l, 0, 0))
    return pl.pallas_call(
        functools.partial(forward_body, n_layers, n_tiles),
        grid=(n_layers, n_tiles + 1),
        in_specs=[
            whole,
            per_layer(rows, e_dim),
            pl.BlockSpec((1, d_model, F_TILE), lambda l, j: (l, 0, jnp.minimum(j, n_tiles - 1))),
            pl.BlockSpec((1, F_TILE, d_model), lambda l, j: (l, jnp.maximum(j - 1, 0), 0)),
            per_layer(d_model, e_dim),
            per_layer(e_dim, d_model),
        ],
        out_specs=[
            whole,
            per_layer(rows, d_model),
            pl.BlockSpec((1, 1, rows, F_TILE), lambda l, j: (l, jnp.minimum(j, n_tiles - 1), 0, 0)),
            per_layer(rows, e_dim),
        ],
        out_shape=[
            jax.ShapeDtypeStruct((rows, d_model), BF16),
            jax.ShapeDtypeStruct((n_layers, rows, d_model), BF16),
            jax.ShapeDtypeStruct((n_layers, n_tiles, rows, F_TILE), F32),
            jax.ShapeDtypeStruct((n_layers, rows, e_dim), F32),
        ],
        scratch_shapes=[pltpu.VMEM((rows, d_model), BF16), pltpu.VMEM((rows, d_model), BF16), pltpu.VMEM((rows, F_TILE), BF16), pltpu.VMEM((rows, d_model), F32)],
        cost_estimate=pl.CostEstimate(flops=4 * n_layers * rows * d_model * ffn, bytes_accessed=n_layers * 40_000_000, transcendentals=0),
        compiler_params=pltpu.CompilerParams(dimension_semantics=('arbitrary', 'arbitrary'), vmem_limit_bytes=56 * 2**20),
        name='forward',
    )(resid_in, fetched, w_up, w_down, w_gate, w_proj)


def backward_body(n_tiles, c_ref, xs_ref, e_ref, gp_ref, dg_ref, wu_ref, wd_ref, wg_ref, wp_ref, cot_ref, gr_ref, dng_s, du_s, acc_s):
    tile = pl.program_id(0)
    chunks = row_chunks(c_ref.shape[0], BWD_CHUNK)

    def hidden_half(r):
        d_hidden = dot_nt(c_ref[r, :], wd_ref[0]).astype(BF16).astype(F32)
        du_s[r, :] = (d_hidden * dg_ref[0, 0, r, :]).astype(BF16)

    @pl.when(tile == 0)
    def _():
        for r in chunks:
            d_mixed = dot_nt(c_ref[r, :], wp_ref[0]).astype(BF16).astype(F32)
            gate_act, slope = gelu_pair(gp_ref[0, r, :])
            gr_ref[r, :] = gate_act * d_mixed
            d_gate = (slope * (d_mixed * e_ref[0, r, :].astype(F32))).astype(BF16)
            dng_s[r, :] = dot_nt(d_gate, wg_ref[0]).astype(BF16)
            acc_s[r, :] = jnp.zeros((r.size, acc_s.shape[1]), F32)
            hidden_half(r)

    @pl.when((tile > 0) & (tile < n_tiles))
    def _():
        for r in chunks:
            acc_s[r, :] += dot_nt(du_s[r, :], wu_ref[0])
            hidden_half(r)

    @pl.when(tile == n_tiles)
    def _():
        for r in chunks:
            acc = acc_s[r, :] + dot_nt(du_s[r, :], wu_ref[0])
            d_n = (acc.astype(BF16).astype(F32) + dng_s[r, :].astype(F32)).astype(BF16).astype(F32)
            x_f = xs_ref[0, r, :].astype(F32)
            inv = lax.rsqrt(jnp.mean(x_f * x_f, axis=-1, keepdims=True) + NORM_EPS)
            proj = jnp.mean(d_n * x_f, axis=-1, keepdims=True)
            d_x = d_n * inv - x_f * (inv * inv * inv * proj)
            cot_ref[r, :] = (c_ref[r, :].astype(F32) + d_x).astype(BF16)


def run_backward(layer, cot, xs, fetched, gp, dg, w_up, w_down, w_gate, w_proj):
    _, d_model, ffn = w_up.shape
    rows, e_dim = cot.shape[0], w_gate.shape[2]
    n_tiles = ffn // F_TILE
    whole = lambda *s: pl.BlockSpec(s, lambda j: (0, 0))
    at_layer = lambda *s: pl.BlockSpec((1,) + s, lambda j: (layer, 0, 0))
    return pl.pallas_call(
        functools.partial(backward_body, n_tiles),
        grid=(n_tiles + 1,),
        in_specs=[
            whole(rows, d_model),
            at_layer(rows, d_model),
            at_layer(rows, e_dim),
            at_layer(rows, e_dim),
            pl.BlockSpec((1, 1, rows, F_TILE), lambda j: (layer, jnp.minimum(j, n_tiles - 1), 0, 0)),
            pl.BlockSpec((1, d_model, F_TILE), lambda j: (layer, 0, jnp.maximum(j - 1, 0))),
            pl.BlockSpec((1, F_TILE, d_model), lambda j: (layer, jnp.minimum(j, n_tiles - 1), 0)),
            at_layer(d_model, e_dim),
            at_layer(e_dim, d_model),
        ],
        out_specs=[whole(rows, d_model), whole(rows, e_dim)],
        out_shape=[jax.ShapeDtypeStruct((rows, d_model), BF16), jax.ShapeDtypeStruct((rows, e_dim), F32)],
        scratch_shapes=[pltpu.VMEM((rows, d_model), BF16), pltpu.VMEM((rows, F_TILE), BF16), pltpu.VMEM((rows, d_model), F32)],
        cost_estimate=pl.CostEstimate(flops=4 * rows * d_model * ffn, bytes_accessed=40_000_000, transcendentals=0),
        compiler_params=pltpu.CompilerParams(dimension_semantics=('arbitrary',), vmem_limit_bytes=56 * 2**20),
        name='backward',
    )(cot, xs, fetched, gp, dg, w_up, w_down, w_gate, w_proj)


def fetch_body(n_layers, n_tok, n_steps, off_ref, table_ref, out_ref, buf, sems):
    step = pl.program_id(0)

    def issue(at, slot):
        def go(i, carry):
            for k in range(8):
                tok = i * 8 + k
                tile = off_ref[at * n_tok + tok] // 8
                pltpu.make_async_copy(table_ref.at[:, pl.ds(pl.multiple_of(tile * 8, 8), 8), :], buf.at[slot, tok], sems.at[slot]).start(priority=k % 2)
            return carry

        lax.fori_loop(0, n_tok // 8, go, 0)

    @pl.when(step == 0)
    def _():
        issue(0, 0)

    @pl.when(step + 1 < n_steps)
    def _():
        issue(step + 1, (step + 1) % 2)

    slot = step % 2
    pltpu.make_async_copy(buf.at[slot], buf.at[slot], sems.at[slot]).wait()
    sub = lax.broadcasted_iota(jnp.int32, (8, 128), 0)

    def pick(i, carry):
        halves = [[None, None] for _ in range(n_layers)]
        for half in range(2):
            for k in range(8):
                tok = i * 16 + half * 8 + k
                shift = (k + 8 - off_ref[step * n_tok + tok] % 8) % 8
                for l in range(n_layers):
                    moved = pltpu.roll(buf[slot, tok, l].astype(F32), shift, axis=0)
                    halves[l][half] = moved if k == 0 else jnp.where(sub == k, moved, halves[l][half])
        for l in range(n_layers):
            out_ref[l, pl.ds(pl.multiple_of(i * 16, 16), 16), :] = jnp.concatenate(halves[l], axis=0).astype(BF16)
        return carry

    lax.fori_loop(0, n_tok // 16, pick, 0)


def run_fetch(tables, offsets):
    n_layers, _, e_dim = tables.shape
    n_rows = offsets.shape[0]
    n_steps = n_rows // FETCH_TOK
    return pl.pallas_call(
        functools.partial(fetch_body, n_layers, FETCH_TOK, n_steps),
        grid_spec=pltpu.PrefetchScalarGridSpec(
            num_scalar_prefetch=1,
            grid=(n_steps,),
            in_specs=[pl.BlockSpec(memory_space=pl.ANY)],
            out_specs=pl.BlockSpec((n_layers, FETCH_TOK, e_dim), lambda i, off: (0, i, 0)),
            scratch_shapes=[pltpu.VMEM((2, FETCH_TOK, n_layers, 8, e_dim), BF16), pltpu.SemaphoreType.DMA((2,))],
        ),
        out_shape=jax.ShapeDtypeStruct((n_layers, n_rows, e_dim), BF16),
        cost_estimate=pl.CostEstimate(flops=2_000_000_000, bytes_accessed=30_000_000, transcendentals=0),
        compiler_params=pltpu.CompilerParams(dimension_semantics=('arbitrary',)),
        name='fetch_rows',
    )(offsets, tables)


def place_body(group, n_group, idx_bits, n_blocks, tail, starts_ref, keys_ref, *refs):
    rows_refs, out_ref, buf, sems = refs[:n_group], refs[-3], refs[-2], refs[-1]
    block = pl.program_id(0)
    slot = block % PLACE_BUFS

    def copy(at, which, rows):
        where = pl.ds(pl.multiple_of(at * OUT_ROWS, OUT_ROWS), rows)
        return pltpu.make_async_copy(buf.at[which, :, pl.ds(0, rows), :], out_ref.at[pl.ds(group * n_group, n_group), where, :], sems.at[which])

    @pl.when(block >= PLACE_BUFS)
    def _():
        copy(block - PLACE_BUFS, slot, OUT_ROWS).wait()

    buf[slot] = jnp.zeros(buf.shape[1:], F32)
    start, end = starts_ref[block], starts_ref[block + 1]
    base = block * OUT_ROWS

    def go(i, carry):
        prev, accs = carry[0], list(carry[1:])
        for u in range(PLACE_UNROLL):
            key = keys_ref[start + i * PLACE_UNROLL + u]
            src = key & ((1 << idx_bits) - 1)
            row_id = key >> idx_bits
            fresh = row_id != prev
            dst = jnp.minimum(row_id - base, OUT_ROWS)
            for g in range(n_group):
                accs[g] = rows_refs[g][pl.ds(src, 1), :] + jnp.where(fresh, 0.0, accs[g])
                buf[slot, g, pl.ds(dst, 1), :] = accs[g]
            prev = row_id
        return (prev, *accs)

    zero = jnp.zeros((1, buf.shape[3]), F32)
    lax.fori_loop(0, (end - start + PLACE_UNROLL - 1) // PLACE_UNROLL, go, (jnp.int32(-1),) + (zero,) * n_group)

    @pl.when(block < n_blocks - 1)
    def _():
        copy(block, slot, OUT_ROWS).start()

    @pl.when(block == n_blocks - 1)
    def _():
        copy(block, slot, tail).start()
        for at in range(max(0, n_blocks - PLACE_BUFS), n_blocks):
            copy(at, at % PLACE_BUFS, tail if at == n_blocks - 1 else OUT_ROWS).wait()


def run_place(group, starts, keys, rows_list, d_tables, shape):
    n_group = len(rows_list)
    n_rows, e_dim = rows_list[0].shape
    idx_bits = (n_rows - 1).bit_length()
    n_blocks = pl.cdiv(shape[1], OUT_ROWS)
    tail = shape[1] - (n_blocks - 1) * OUT_ROWS
    args = [starts, keys, *rows_list]
    in_specs = [pl.BlockSpec((n_rows, e_dim), lambda i, s, k: (0, 0)) for _ in rows_list]
    aliases = {}
    if d_tables is not None:
        aliases = {len(args): 0}
        args.append(d_tables)
        in_specs.append(pl.BlockSpec(memory_space=pl.ANY))
    return pl.pallas_call(
        functools.partial(place_body, group, n_group, idx_bits, n_blocks, tail),
        grid_spec=pltpu.PrefetchScalarGridSpec(
            num_scalar_prefetch=2,
            grid=(n_blocks,),
            in_specs=in_specs,
            out_specs=pl.BlockSpec(memory_space=pl.ANY),
            scratch_shapes=[pltpu.VMEM((PLACE_BUFS, n_group, OUT_ROWS + 8, e_dim), F32), pltpu.SemaphoreType.DMA((PLACE_BUFS,))],
        ),
        out_shape=jax.ShapeDtypeStruct(shape, F32),
        input_output_aliases=aliases,
        cost_estimate=pl.CostEstimate(flops=30_000_000_000, bytes_accessed=n_group * 44_000_000, transcendentals=0),
        compiler_params=pltpu.CompilerParams(dimension_semantics=('arbitrary',), vmem_limit_bytes=56 * 2**20),
        name='place_rows',
    )(*args)


def solution(mesh):
    n_emb = mesh.shape['emb']
    tok_spec = P(('dp', 'emb'))
    act_spec = P(('dp', 'emb'), None)
    table_spec = P(None, 'emb', None)
    full_spec = P(None, None, None)
    swap = [(i, (i + 1) % n_emb) for i in range(n_emb)]

    def device_body(tok_ids, resid_in, cot_out, tables, w_up, w_down, w_gate, w_proj):
        n_layers, range_rows, e_dim = tables.shape
        tok_count = tok_ids.shape[0]
        base = lax.axis_index('emb') * range_rows

        own_off = tok_ids - base
        own_mask = (own_off >= 0) & (own_off < range_rows)
        peer_ids = lax.ppermute(tok_ids, 'emb', swap)
        pair_off = jnp.concatenate([own_off, peer_ids - base])
        spread = (jnp.arange(pair_off.shape[0], dtype=jnp.int32) * 32) % range_rows
        offsets = jnp.where((pair_off >= 0) & (pair_off < range_rows), pair_off, spread)
        served = run_fetch(tables, offsets)
        from_peer = lax.ppermute(served[:, tok_count:], 'emb', swap)
        fetched = jnp.where(own_mask[None, :, None], served[:, :tok_count], from_peer)

        all_ids = lax.all_gather(tok_ids, ('dp', 'emb'), axis=0, tiled=True)
        n_all = all_ids.shape[0]
        idx_bits = (n_all - 1).bit_length()
        all_off = all_ids - base
        all_off = jnp.where((all_off >= 0) & (all_off < range_rows), all_off, range_rows)
        keys = jnp.sort((all_off << idx_bits) | jnp.arange(n_all, dtype=jnp.int32))
        n_blocks = pl.cdiv(range_rows, OUT_ROWS)
        pad = jnp.full((PLACE_UNROLL,), range_rows << idx_bits, jnp.int32)
        bounds = jnp.minimum(jnp.arange(n_blocks + 1, dtype=jnp.int32) * OUT_ROWS, range_rows)
        starts = jnp.sum((all_off[None, :] < bounds[:, None]).astype(jnp.int32), axis=1)

        keys = jnp.concatenate([keys, pad])
        keys, starts, fetched = lax.optimization_barrier((keys, starts, fetched))

        resid_out, xs, dg, gp = run_forward(resid_in, fetched, w_up, w_down, w_gate, w_proj)

        cot = cot_out
        rows_list = [None] * n_layers
        for layer in reversed(range(n_layers)):
            cot, grad_rows = run_backward(layer, cot, xs, fetched, gp, dg, w_up, w_down, w_gate, w_proj)
            if layer == 0:
                grad_rows, rows_list[1] = lax.optimization_barrier((grad_rows, rows_list[1]))
            rows_list[layer] = lax.all_gather(grad_rows, ('dp', 'emb'), axis=0, tiled=True)

        d_tables = None
        per_group = n_layers // 2
        for group in (1, 0):
            d_tables = run_place(group, starts, keys, rows_list[group * per_group:(group + 1) * per_group], d_tables, tables.shape)
        return resid_out, d_tables

    return jax.shard_map(device_body, mesh=mesh, in_specs=(tok_spec, act_spec, act_spec, table_spec, full_spec, full_spec, full_spec, full_spec), out_specs=(act_spec, table_spec), check_vma=False)
```

```python
import functools

import jax
import jax.numpy as jnp
from jax import lax
from jax.experimental import pallas as pl
from jax.experimental.pallas import tpu as pltpu
from jax.sharding import PartitionSpec as P

NORM_EPS = 1e-6
GELU_K = 0.7978845608028654
GELU_A = 0.044715
F_TILE = 256
FWD_CHUNK = 256
BWD_CHUNK = 1024
OUT_ROWS = 1024
PLACE_UNROLL = 8
PLACE_BUFS = 4
FETCH_TOK = 128
F32 = jnp.float32
BF16 = jnp.bfloat16


def gelu_pair(x):
    sq = x * x
    t = jnp.tanh(x * (GELU_K + (GELU_K * GELU_A) * sq))
    cdf = 0.5 + 0.5 * t
    slope = cdf + (0.5 * x) * (1.0 - t * t) * (GELU_K + (3.0 * GELU_K * GELU_A) * sq)
    return x * cdf, slope


def dot_nn(a, b):
    return lax.dot_general(a, b, (((1,), (0,)), ((), ())), preferred_element_type=F32)


def dot_nt(a, b):
    return lax.dot_general(a, b, (((1,), (1,)), ((), ())), preferred_element_type=F32)


def row_chunks(rows, size):
    return [pl.ds(r, min(size, rows)) for r in range(0, rows, size)]


def forward_body(n_layers, n_tiles, x_ref, e_ref, wu_ref, wd_ref, wg_ref, wp_ref, out_ref, xs_ref, dg_ref, gp_ref, x_s, u_s, h_s, acc_s):
    layer, tile = pl.program_id(0), pl.program_id(1)
    chunks = row_chunks(x_s.shape[0], FWD_CHUNK)

    def up_half(r):
        act, slope = gelu_pair(dot_nn(u_s[r, :], wu_ref[0]))
        dg_ref[0, 0, r, :] = slope
        h_s[r, :] = act.astype(BF16)

    def down_half(r):
        acc_s[r, :] += dot_nn(h_s[r, :], wd_ref[0])

    @pl.when((layer == 0) & (tile == 0))
    def _():
        x_s[...] = x_ref[...]

    @pl.when(tile == 0)
    def _():
        for r in chunks:
            x_bf = x_s[r, :]
            xs_ref[0, r, :] = x_bf
            x_f = x_bf.astype(F32)
            u = (x_f * lax.rsqrt(jnp.mean(x_f * x_f, axis=-1, keepdims=True) + NORM_EPS)).astype(BF16)
            u_s[r, :] = u
            gate_pre = dot_nn(u, wg_ref[0])
            gp_ref[0, r, :] = gate_pre
            gate_act, _ = gelu_pair(gate_pre)
            mixed = (gate_act * e_ref[0, r, :].astype(F32)).astype(BF16)
            acc_s[r, :] = x_f + dot_nn(mixed, wp_ref[0])
            up_half(r)

    @pl.when((tile > 0) & (tile < n_tiles))
    def _():
        for r in chunks:
            down_half(r)
            up_half(r)

    @pl.when(tile == n_tiles)
    def _():
        for r in chunks:
            x_s[r, :] = (acc_s[r, :] + dot_nn(h_s[r, :], wd_ref[0])).astype(BF16)

    @pl.when((tile == n_tiles) & (layer == n_layers - 1))
    def _():
        out_ref[...] = x_s[...]


def run_forward(resid_in, fetched, w_up, w_down, w_gate, w_proj):
    n_layers, d_model, ffn = w_up.shape
    rows, e_dim = resid_in.shape[0], w_gate.shape[2]
    n_tiles = ffn // F_TILE
    whole = pl.BlockSpec((rows, d_model), lambda l, j: (0, 0))
    per_layer = lambda *s: pl.BlockSpec((1,) + s, lambda l, j: (l, 0, 0))
    return pl.pallas_call(
        functools.partial(forward_body, n_layers, n_tiles),
        grid=(n_layers, n_tiles + 1),
        in_specs=[
            whole,
            per_layer(rows, e_dim),
            pl.BlockSpec((1, d_model, F_TILE), lambda l, j: (l, 0, jnp.minimum(j, n_tiles - 1))),
            pl.BlockSpec((1, F_TILE, d_model), lambda l, j: (l, jnp.maximum(j - 1, 0), 0)),
            per_layer(d_model, e_dim),
            per_layer(e_dim, d_model),
        ],
        out_specs=[
            whole,
            per_layer(rows, d_model),
            pl.BlockSpec((1, 1, rows, F_TILE), lambda l, j: (l, jnp.minimum(j, n_tiles - 1), 0, 0)),
            per_layer(rows, e_dim),
        ],
        out_shape=[
            jax.ShapeDtypeStruct((rows, d_model), BF16),
            jax.ShapeDtypeStruct((n_layers, rows, d_model), BF16),
            jax.ShapeDtypeStruct((n_layers, n_tiles, rows, F_TILE), F32),
            jax.ShapeDtypeStruct((n_layers, rows, e_dim), F32),
        ],
        scratch_shapes=[pltpu.VMEM((rows, d_model), BF16), pltpu.VMEM((rows, d_model), BF16), pltpu.VMEM((rows, F_TILE), BF16), pltpu.VMEM((rows, d_model), F32)],
        cost_estimate=pl.CostEstimate(flops=4 * n_layers * rows * d_model * ffn, bytes_accessed=n_layers * 40_000_000, transcendentals=0),
        compiler_params=pltpu.CompilerParams(dimension_semantics=('arbitrary', 'arbitrary'), vmem_limit_bytes=56 * 2**20),
        name='forward',
    )(resid_in, fetched, w_up, w_down, w_gate, w_proj)


def backward_body(n_tiles, c_ref, xs_ref, e_ref, gp_ref, dg_ref, wu_ref, wd_ref, wg_ref, wp_ref, cot_ref, gr_ref, dng_s, du_s, acc_s):
    tile = pl.program_id(0)
    chunks = row_chunks(c_ref.shape[0], BWD_CHUNK)

    def hidden_half(r):
        d_hidden = dot_nt(c_ref[r, :], wd_ref[0]).astype(BF16).astype(F32)
        du_s[r, :] = (d_hidden * dg_ref[0, 0, r, :]).astype(BF16)

    @pl.when(tile == 0)
    def _():
        for r in chunks:
            d_mixed = dot_nt(c_ref[r, :], wp_ref[0]).astype(BF16).astype(F32)
            gate_act, slope = gelu_pair(gp_ref[0, r, :])
            gr_ref[r, :] = gate_act * d_mixed
            d_gate = (slope * (d_mixed * e_ref[0, r, :].astype(F32))).astype(BF16)
            dng_s[r, :] = dot_nt(d_gate, wg_ref[0]).astype(BF16)
            acc_s[r, :] = jnp.zeros((r.size, acc_s.shape[1]), F32)
            hidden_half(r)

    @pl.when((tile > 0) & (tile < n_tiles))
    def _():
        for r in chunks:
            acc_s[r, :] += dot_nt(du_s[r, :], wu_ref[0])
            hidden_half(r)

    @pl.when(tile == n_tiles)
    def _():
        for r in chunks:
            acc = acc_s[r, :] + dot_nt(du_s[r, :], wu_ref[0])
            d_n = (acc.astype(BF16).astype(F32) + dng_s[r, :].astype(F32)).astype(BF16).astype(F32)
            x_f = xs_ref[0, r, :].astype(F32)
            inv = lax.rsqrt(jnp.mean(x_f * x_f, axis=-1, keepdims=True) + NORM_EPS)
            proj = jnp.mean(d_n * x_f, axis=-1, keepdims=True)
            d_x = d_n * inv - x_f * (inv * inv * inv * proj)
            cot_ref[r, :] = (c_ref[r, :].astype(F32) + d_x).astype(BF16)


def run_backward(layer, cot, xs, fetched, gp, dg, w_up, w_down, w_gate, w_proj):
    _, d_model, ffn = w_up.shape
    rows, e_dim = cot.shape[0], w_gate.shape[2]
    n_tiles = ffn // F_TILE
    whole = lambda *s: pl.BlockSpec(s, lambda j: (0, 0))
    at_layer = lambda *s: pl.BlockSpec((1,) + s, lambda j: (layer, 0, 0))
    return pl.pallas_call(
        functools.partial(backward_body, n_tiles),
        grid=(n_tiles + 1,),
        in_specs=[
            whole(rows, d_model),
            at_layer(rows, d_model),
            at_layer(rows, e_dim),
            at_layer(rows, e_dim),
            pl.BlockSpec((1, 1, rows, F_TILE), lambda j: (layer, jnp.minimum(j, n_tiles - 1), 0, 0)),
            pl.BlockSpec((1, d_model, F_TILE), lambda j: (layer, 0, jnp.maximum(j - 1, 0))),
            pl.BlockSpec((1, F_TILE, d_model), lambda j: (layer, jnp.minimum(j, n_tiles - 1), 0)),
            at_layer(d_model, e_dim),
            at_layer(e_dim, d_model),
        ],
        out_specs=[whole(rows, d_model), whole(rows, e_dim)],
        out_shape=[jax.ShapeDtypeStruct((rows, d_model), BF16), jax.ShapeDtypeStruct((rows, e_dim), F32)],
        scratch_shapes=[pltpu.VMEM((rows, d_model), BF16), pltpu.VMEM((rows, F_TILE), BF16), pltpu.VMEM((rows, d_model), F32)],
        cost_estimate=pl.CostEstimate(flops=4 * rows * d_model * ffn, bytes_accessed=40_000_000, transcendentals=0),
        compiler_params=pltpu.CompilerParams(dimension_semantics=('arbitrary',), vmem_limit_bytes=56 * 2**20),
        name='backward',
    )(cot, xs, fetched, gp, dg, w_up, w_down, w_gate, w_proj)


def fetch_body(n_layers, n_tok, n_steps, off_ref, table_ref, out_ref, buf, sems):
    step = pl.program_id(0)

    def issue(at, slot):
        def go(i, carry):
            for k in range(8):
                tok = i * 8 + k
                tile = off_ref[at * n_tok + tok] // 8
                pltpu.make_async_copy(table_ref.at[:, pl.ds(pl.multiple_of(tile * 8, 8), 8), :], buf.at[slot, tok], sems.at[slot]).start(priority=k % 2)
            return carry

        lax.fori_loop(0, n_tok // 8, go, 0)

    @pl.when(step == 0)
    def _():
        issue(0, 0)

    @pl.when(step + 1 < n_steps)
    def _():
        issue(step + 1, (step + 1) % 2)

    slot = step % 2
    pltpu.make_async_copy(buf.at[slot], buf.at[slot], sems.at[slot]).wait()
    sub = lax.broadcasted_iota(jnp.int32, (8, 128), 0)

    def pick(i, carry):
        halves = [[None, None] for _ in range(n_layers)]
        for half in range(2):
            for k in range(8):
                tok = i * 16 + half * 8 + k
                shift = (k + 8 - off_ref[step * n_tok + tok] % 8) % 8
                for l in range(n_layers):
                    moved = pltpu.roll(buf[slot, tok, l].astype(F32), shift, axis=0)
                    halves[l][half] = moved if k == 0 else jnp.where(sub == k, moved, halves[l][half])
        for l in range(n_layers):
            out_ref[l, pl.ds(pl.multiple_of(i * 16, 16), 16), :] = jnp.concatenate(halves[l], axis=0).astype(BF16)
        return carry

    lax.fori_loop(0, n_tok // 16, pick, 0)


def run_fetch(tables, offsets):
    n_layers, _, e_dim = tables.shape
    n_rows = offsets.shape[0]
    n_steps = n_rows // FETCH_TOK
    return pl.pallas_call(
        functools.partial(fetch_body, n_layers, FETCH_TOK, n_steps),
        grid_spec=pltpu.PrefetchScalarGridSpec(
            num_scalar_prefetch=1,
            grid=(n_steps,),
            in_specs=[pl.BlockSpec(memory_space=pl.ANY)],
            out_specs=pl.BlockSpec((n_layers, FETCH_TOK, e_dim), lambda i, off: (0, i, 0)),
            scratch_shapes=[pltpu.VMEM((2, FETCH_TOK, n_layers, 8, e_dim), BF16), pltpu.SemaphoreType.DMA((2,))],
        ),
        out_shape=jax.ShapeDtypeStruct((n_layers, n_rows, e_dim), BF16),
        cost_estimate=pl.CostEstimate(flops=2_000_000_000, bytes_accessed=30_000_000, transcendentals=0),
        compiler_params=pltpu.CompilerParams(dimension_semantics=('arbitrary',)),
        name='fetch_rows',
    )(offsets, tables)


def place_body(group, n_group, idx_bits, n_blocks, tail, starts_ref, keys_ref, *refs):
    rows_refs, out_ref, buf, sems = refs[:n_group], refs[-3], refs[-2], refs[-1]
    block = pl.program_id(0)
    slot = block % PLACE_BUFS

    def copy(at, which, rows):
        where = pl.ds(pl.multiple_of(at * OUT_ROWS, OUT_ROWS), rows)
        return pltpu.make_async_copy(buf.at[which, :, pl.ds(0, rows), :], out_ref.at[pl.ds(group * n_group, n_group), where, :], sems.at[which])

    @pl.when(block >= PLACE_BUFS)
    def _():
        copy(block - PLACE_BUFS, slot, OUT_ROWS).wait()

    buf[slot] = jnp.zeros(buf.shape[1:], F32)
    start, end = starts_ref[block], starts_ref[block + 1]
    base = block * OUT_ROWS

    def go(i, carry):
        prev, accs = carry[0], list(carry[1:])
        for u in range(PLACE_UNROLL):
            key = keys_ref[start + i * PLACE_UNROLL + u]
            src = key & ((1 << idx_bits) - 1)
            row_id = key >> idx_bits
            fresh = row_id != prev
            dst = jnp.minimum(row_id - base, OUT_ROWS)
            for g in range(n_group):
                accs[g] = rows_refs[g][pl.ds(src, 1), :] + jnp.where(fresh, 0.0, accs[g])
                buf[slot, g, pl.ds(dst, 1), :] = accs[g]
            prev = row_id
        return (prev, *accs)

    zero = jnp.zeros((1, buf.shape[3]), F32)
    lax.fori_loop(0, (end - start + PLACE_UNROLL - 1) // PLACE_UNROLL, go, (jnp.int32(-1),) + (zero,) * n_group)

    @pl.when(block < n_blocks - 1)
    def _():
        copy(block, slot, OUT_ROWS).start()

    @pl.when(block == n_blocks - 1)
    def _():
        copy(block, slot, tail).start()
        for at in range(max(0, n_blocks - PLACE_BUFS), n_blocks):
            copy(at, at % PLACE_BUFS, tail if at == n_blocks - 1 else OUT_ROWS).wait()


def run_place(group, starts, keys, rows_list, d_tables, shape):
    n_group = len(rows_list)
    n_rows, e_dim = rows_list[0].shape
    idx_bits = (n_rows - 1).bit_length()
    n_blocks = pl.cdiv(shape[1], OUT_ROWS)
    tail = shape[1] - (n_blocks - 1) * OUT_ROWS
    args = [starts, keys, *rows_list]
    in_specs = [pl.BlockSpec((n_rows, e_dim), lambda i, s, k: (0, 0)) for _ in rows_list]
    aliases = {}
    if d_tables is not None:
        aliases = {len(args): 0}
        args.append(d_tables)
        in_specs.append(pl.BlockSpec(memory_space=pl.ANY))
    return pl.pallas_call(
        functools.partial(place_body, group, n_group, idx_bits, n_blocks, tail),
        grid_spec=pltpu.PrefetchScalarGridSpec(
            num_scalar_prefetch=2,
            grid=(n_blocks,),
            in_specs=in_specs,
            out_specs=pl.BlockSpec(memory_space=pl.ANY),
            scratch_shapes=[pltpu.VMEM((PLACE_BUFS, n_group, OUT_ROWS + 8, e_dim), F32), pltpu.SemaphoreType.DMA((PLACE_BUFS,))],
        ),
        out_shape=jax.ShapeDtypeStruct(shape, F32),
        input_output_aliases=aliases,
        cost_estimate=pl.CostEstimate(flops=30_000_000_000, bytes_accessed=n_group * 44_000_000, transcendentals=0),
        compiler_params=pltpu.CompilerParams(dimension_semantics=('arbitrary',), vmem_limit_bytes=56 * 2**20),
        name='place_rows',
    )(*args)


def solution(mesh):
    n_emb = mesh.shape['emb']
    tok_spec = P(('dp', 'emb'))
    act_spec = P(('dp', 'emb'), None)
    table_spec = P(None, 'emb', None)
    full_spec = P(None, None, None)
    swap = [(i, (i + 1) % n_emb) for i in range(n_emb)]

    def device_body(tok_ids, resid_in, cot_out, tables, w_up, w_down, w_gate, w_proj):
        n_layers, range_rows, e_dim = tables.shape
        tok_count = tok_ids.shape[0]
        base = lax.axis_index('emb') * range_rows

        own_off = tok_ids - base
        own_mask = (own_off >= 0) & (own_off < range_rows)
        peer_ids = lax.ppermute(tok_ids, 'emb', swap)
        pair_off = jnp.concatenate([own_off, peer_ids - base])
        spread = (jnp.arange(pair_off.shape[0], dtype=jnp.int32) * 32) % range_rows
        offsets = jnp.where((pair_off >= 0) & (pair_off < range_rows), pair_off, spread)
        served = run_fetch(tables, offsets)
        from_peer = lax.ppermute(served[:, tok_count:], 'emb', swap)
        fetched = jnp.where(own_mask[None, :, None], served[:, :tok_count], from_peer)

        all_ids = lax.all_gather(tok_ids, ('dp', 'emb'), axis=0, tiled=True)
        n_all = all_ids.shape[0]
        idx_bits = (n_all - 1).bit_length()
        all_off = all_ids - base
        all_off = jnp.where((all_off >= 0) & (all_off < range_rows), all_off, range_rows)
        keys = jnp.sort((all_off << idx_bits) | jnp.arange(n_all, dtype=jnp.int32))
        n_blocks = pl.cdiv(range_rows, OUT_ROWS)
        pad = jnp.full((PLACE_UNROLL,), range_rows << idx_bits, jnp.int32)
        bounds = jnp.minimum(jnp.arange(n_blocks + 1, dtype=jnp.int32) * OUT_ROWS, range_rows)
        starts = jnp.sum((all_off[None, :] < bounds[:, None]).astype(jnp.int32), axis=1)

        keys = jnp.concatenate([keys, pad])
        keys, starts, fetched = lax.optimization_barrier((keys, starts, fetched))

        resid_out, xs, dg, gp = run_forward(resid_in, fetched, w_up, w_down, w_gate, w_proj)

        cot = cot_out
        rows_list = [None] * n_layers
        for layer in reversed(range(n_layers)):
            if layer + 2 < n_layers:
                cot, rows_list[layer + 2] = lax.optimization_barrier((cot, rows_list[layer + 2]))
            cot, grad_rows = run_backward(layer, cot, xs, fetched, gp, dg, w_up, w_down, w_gate, w_proj)
            if layer == 0:
                grad_rows, rows_list[1] = lax.optimization_barrier((grad_rows, rows_list[1]))
            rows_list[layer] = lax.all_gather(grad_rows, ('dp', 'emb'), axis=0, tiled=True)

        d_tables = None
        per_group = n_layers // 2
        for group in (1, 0):
            d_tables = run_place(group, starts, keys, rows_list[group * per_group:(group + 1) * per_group], d_tables, tables.shape)
        return resid_out, d_tables

    return jax.shard_map(device_body, mesh=mesh, in_specs=(tok_spec, act_spec, act_spec, table_spec, full_spec, full_spec, full_spec, full_spec), out_specs=(act_spec, table_spec), check_vma=False)
```

```python
import functools

import jax
import jax.numpy as jnp
from jax import lax
from jax.experimental import pallas as pl
from jax.experimental.pallas import tpu as pltpu
from jax.sharding import PartitionSpec as P

NORM_EPS = 1e-6
GELU_K = 0.7978845608028654
GELU_A = 0.044715
F_TILE = 256
RING = 6
SLOPE_RING = 4
FWD_CHUNK = 256
BWD_CHUNK = 1024
OUT_ROWS = 1024
PLACE_UNROLL = 8
PLACE_BUFS = 12
FETCH_TOK = 128
F32 = jnp.float32
BF16 = jnp.bfloat16


def gelu_pair(x):
    sq = x * x
    t = jnp.tanh(x * (GELU_K + (GELU_K * GELU_A) * sq))
    cdf = 0.5 + 0.5 * t
    slope = cdf + (0.5 * x) * (1.0 - t * t) * (GELU_K + (3.0 * GELU_K * GELU_A) * sq)
    return x * cdf, slope


def dot_nn(a, b):
    return lax.dot_general(a, b, (((1,), (0,)), ((), ())), preferred_element_type=F32)


def dot_nt(a, b):
    return lax.dot_general(a, b, (((1,), (1,)), ((), ())), preferred_element_type=F32)


def row_chunks(rows, size):
    return [pl.ds(r, min(size, rows)) for r in range(0, rows, size)]


def weight_copy(src, buf, sems, layer, tile, index, by_rows):
    span = pl.ds(pl.multiple_of(tile * F_TILE, F_TILE), F_TILE)
    part = src.at[layer, span, :] if by_rows else src.at[layer, :, span]
    slot = index % RING
    return pltpu.make_async_copy(part, buf.at[slot], sems.at[slot])


def forward_body(n_layers, n_tiles, x_ref, e_ref, wu_ref, wd_ref, wg_ref, wp_ref, out_ref, xs_ref, dg_ref, gp_ref, x_s, u_s, h_s, acc_s, wu_s, wd_s, dg_s, wu_sem, wd_sem, dg_sem):
    layer = pl.program_id(0)
    chunks = row_chunks(x_s.shape[0], FWD_CHUNK)
    total = n_layers * n_tiles
    first = layer * n_tiles

    def up_copy(i):
        return weight_copy(wu_ref, wu_s, wu_sem, i // n_tiles, i % n_tiles, i, False)

    def down_copy(i):
        return weight_copy(wd_ref, wd_s, wd_sem, i // n_tiles, i % n_tiles, i, True)

    def slope_copy(i):
        return pltpu.make_async_copy(dg_s.at[i % SLOPE_RING], dg_ref.at[i // n_tiles, i % n_tiles], dg_sem.at[i % SLOPE_RING])

    def enter(i):
        @pl.when(i + RING - 1 < total)
        def _():
            up_copy(i + RING - 1).start()

        @pl.when(i + RING - 2 < total)
        def _():
            down_copy(i + RING - 2).start()

        @pl.when(i + 1 < total)
        def _():
            up_copy(i + 1).wait()

        down_copy(i).wait()

        @pl.when(i >= SLOPE_RING)
        def _():
            slope_copy(i - SLOPE_RING).wait()

    def up_half(i, r):
        act, slope = gelu_pair(dot_nn(u_s[r, :], wu_s[i % RING]))
        dg_s[i % SLOPE_RING, r, :] = slope
        h_s[r, :] = act.astype(BF16)

    @pl.when(layer == 0)
    def _():
        for i in range(min(RING - 1, total)):
            up_copy(i).start()
            if i < RING - 2:
                down_copy(i).start()
        x_s[...] = x_ref[...]
        up_copy(0).wait()

    enter(first)
    for r in chunks:
        x_bf = x_s[r, :]
        xs_ref[0, r, :] = x_bf
        x_f = x_bf.astype(F32)
        u = (x_f * lax.rsqrt(jnp.mean(x_f * x_f, axis=-1, keepdims=True) + NORM_EPS)).astype(BF16)
        u_s[r, :] = u
        gate_pre = dot_nn(u, wg_ref[0])
        gp_ref[0, r, :] = gate_pre
        gate_act, _ = gelu_pair(gate_pre)
        mixed = (gate_act * e_ref[0, r, :].astype(F32)).astype(BF16)
        acc_s[r, :] = x_f + dot_nn(mixed, wp_ref[0])
        up_half(first, r)
    slope_copy(first).start()

    def tile_step(tile, carry):
        i = first + tile
        enter(i)
        for r in chunks:
            acc_s[r, :] += dot_nn(h_s[r, :], wd_s[(i - 1) % RING])
            up_half(i, r)
        slope_copy(i).start()
        return carry

    lax.fori_loop(1, n_tiles, tile_step, 0)
    for r in chunks:
        x_s[r, :] = (acc_s[r, :] + dot_nn(h_s[r, :], wd_s[(first + n_tiles - 1) % RING])).astype(BF16)

    @pl.when(layer == n_layers - 1)
    def _():
        out_ref[...] = x_s[...]
        for i in range(max(0, total - SLOPE_RING), total):
            slope_copy(i).wait()


def run_forward(resid_in, fetched, w_up, w_down, w_gate, w_proj):
    n_layers, d_model, ffn = w_up.shape
    rows, e_dim = resid_in.shape[0], w_gate.shape[2]
    n_tiles = ffn // F_TILE
    whole = pl.BlockSpec((rows, d_model), lambda l: (0, 0))
    in_hbm = pl.BlockSpec(memory_space=pl.ANY)
    per_layer = lambda *s: pl.BlockSpec((1,) + s, lambda l: (l, 0, 0))
    return pl.pallas_call(
        functools.partial(forward_body, n_layers, n_tiles),
        grid=(n_layers,),
        in_specs=[whole, per_layer(rows, e_dim), in_hbm, in_hbm, per_layer(d_model, e_dim), per_layer(e_dim, d_model)],
        out_specs=[whole, per_layer(rows, d_model), in_hbm, per_layer(rows, e_dim)],
        out_shape=[
            jax.ShapeDtypeStruct((rows, d_model), BF16),
            jax.ShapeDtypeStruct((n_layers, rows, d_model), BF16),
            jax.ShapeDtypeStruct((n_layers, n_tiles, rows, F_TILE), F32),
            jax.ShapeDtypeStruct((n_layers, rows, e_dim), F32),
        ],
        scratch_shapes=[
            pltpu.VMEM((rows, d_model), BF16),
            pltpu.VMEM((rows, d_model), BF16),
            pltpu.VMEM((rows, F_TILE), BF16),
            pltpu.VMEM((rows, d_model), F32),
            pltpu.VMEM((RING, d_model, F_TILE), BF16),
            pltpu.VMEM((RING, F_TILE, d_model), BF16),
            pltpu.VMEM((SLOPE_RING, rows, F_TILE), F32),
            pltpu.SemaphoreType.DMA((RING,)),
            pltpu.SemaphoreType.DMA((RING,)),
            pltpu.SemaphoreType.DMA((SLOPE_RING,)),
        ],
        cost_estimate=pl.CostEstimate(flops=4 * n_layers * rows * d_model * ffn, bytes_accessed=n_layers * 40_000_000, transcendentals=0),
        compiler_params=pltpu.CompilerParams(dimension_semantics=('arbitrary',), vmem_limit_bytes=56 * 2**20),
        name='forward',
    )(resid_in, fetched, w_up, w_down, w_gate, w_proj)


def backward_body(layer, n_tiles, c_ref, xs_ref, e_ref, gp_ref, dg_ref, wu_ref, wd_ref, wg_ref, wp_ref, cot_ref, gr_ref, xs_s, dng_s, du_s, acc_s, wu_s, wd_s, dg_s, wu_sem, wd_sem, dg_sem, xs_sem):
    chunks = row_chunks(c_ref.shape[0], BWD_CHUNK)

    def up_copy(i):
        return weight_copy(wu_ref, wu_s, wu_sem, layer, i, i, False)

    def down_copy(i):
        return weight_copy(wd_ref, wd_s, wd_sem, layer, i, i, True)

    def slope_copy(i):
        return pltpu.make_async_copy(dg_ref.at[layer, i], dg_s.at[i % RING], dg_sem.at[i % RING])

    saved_copy = pltpu.make_async_copy(xs_ref.at[layer], xs_s, xs_sem)

    def enter(i):
        @pl.when(i + RING - 1 < n_tiles)
        def _():
            down_copy(i + RING - 1).start()
            slope_copy(i + RING - 1).start()

        @pl.when(i + RING - 2 < n_tiles)
        def _():
            up_copy(i + RING - 2).start()

        @pl.when(i + 1 < n_tiles)
        def _():
            down_copy(i + 1).wait()
            slope_copy(i + 1).wait()

        up_copy(i).wait()

    def hidden_half(i, r):
        d_hidden = dot_nt(c_ref[r, :], wd_s[i % RING]).astype(BF16).astype(F32)
        du_s[r, :] = (d_hidden * dg_s[i % RING, r, :]).astype(BF16)

    for i in range(min(RING - 1, n_tiles)):
        down_copy(i).start()
        slope_copy(i).start()
        if i < RING - 2:
            up_copy(i).start()
    saved_copy.start()
    down_copy(0).wait()
    slope_copy(0).wait()
    enter(0)
    for r in chunks:
        d_mixed = dot_nt(c_ref[r, :], wp_ref[0]).astype(BF16).astype(F32)
        gate_act, slope = gelu_pair(gp_ref[0, r, :])
        gr_ref[r, :] = gate_act * d_mixed
        d_gate = (slope * (d_mixed * e_ref[0, r, :].astype(F32))).astype(BF16)
        dng_s[r, :] = dot_nt(d_gate, wg_ref[0]).astype(BF16)
        acc_s[r, :] = jnp.zeros((r.size, acc_s.shape[1]), F32)
        hidden_half(0, r)

    def tile_step(i, carry):
        enter(i)
        for r in chunks:
            acc_s[r, :] += dot_nt(du_s[r, :], wu_s[(i - 1) % RING])
            hidden_half(i, r)
        return carry

    lax.fori_loop(1, n_tiles, tile_step, 0)
    saved_copy.wait()
    for r in row_chunks(c_ref.shape[0], FWD_CHUNK):
        acc = acc_s[r, :] + dot_nt(du_s[r, :], wu_s[(n_tiles - 1) % RING])
        d_n = (acc.astype(BF16).astype(F32) + dng_s[r, :].astype(F32)).astype(BF16).astype(F32)
        x_f = xs_s[r, :].astype(F32)
        inv = lax.rsqrt(jnp.mean(x_f * x_f, axis=-1, keepdims=True) + NORM_EPS)
        proj = jnp.mean(d_n * x_f, axis=-1, keepdims=True)
        d_x = d_n * inv - x_f * (inv * inv * inv * proj)
        cot_ref[r, :] = (c_ref[r, :].astype(F32) + d_x).astype(BF16)


def run_backward(layer, cot, xs, fetched, gp, dg, w_up, w_down, w_gate, w_proj):
    _, d_model, ffn = w_up.shape
    rows, e_dim = cot.shape[0], w_gate.shape[2]
    n_tiles = ffn // F_TILE
    whole = lambda *s: pl.BlockSpec(s, lambda j: (0, 0))
    in_hbm = pl.BlockSpec(memory_space=pl.ANY)
    at_layer = lambda *s: pl.BlockSpec((1,) + s, lambda j: (layer, 0, 0))
    return pl.pallas_call(
        functools.partial(backward_body, layer, n_tiles),
        grid=(1,),
        in_specs=[whole(rows, d_model), in_hbm, at_layer(rows, e_dim), at_layer(rows, e_dim), in_hbm, in_hbm, in_hbm, at_layer(d_model, e_dim), at_layer(e_dim, d_model)],
        out_specs=[whole(rows, d_model), whole(rows, e_dim)],
        out_shape=[jax.ShapeDtypeStruct((rows, d_model), BF16), jax.ShapeDtypeStruct((rows, e_dim), F32)],
        scratch_shapes=[
            pltpu.VMEM((rows, d_model), BF16),
            pltpu.VMEM((rows, d_model), BF16),
            pltpu.VMEM((rows, F_TILE), BF16),
            pltpu.VMEM((rows, d_model), F32),
            pltpu.VMEM((RING, d_model, F_TILE), BF16),
            pltpu.VMEM((RING, F_TILE, d_model), BF16),
            pltpu.VMEM((RING, rows, F_TILE), F32),
            pltpu.SemaphoreType.DMA((RING,)),
            pltpu.SemaphoreType.DMA((RING,)),
            pltpu.SemaphoreType.DMA((RING,)),
            pltpu.SemaphoreType.DMA,
        ],
        cost_estimate=pl.CostEstimate(flops=4 * rows * d_model * ffn, bytes_accessed=40_000_000, transcendentals=0),
        compiler_params=pltpu.CompilerParams(dimension_semantics=('arbitrary',), vmem_limit_bytes=56 * 2**20),
        name='backward',
    )(cot, xs, fetched, gp, dg, w_up, w_down, w_gate, w_proj)


def fetch_body(n_layers, n_tok, n_steps, off_ref, table_ref, out_ref, buf, sems):
    step = pl.program_id(0)

    def issue(at, slot):
        def go(i, carry):
            for k in range(8):
                tok = i * 8 + k
                tile = off_ref[at * n_tok + tok] // 8
                pltpu.make_async_copy(table_ref.at[:, pl.ds(pl.multiple_of(tile * 8, 8), 8), :], buf.at[slot, tok], sems.at[slot]).start(priority=k % 2)
            return carry

        lax.fori_loop(0, n_tok // 8, go, 0)

    @pl.when(step == 0)
    def _():
        issue(0, 0)

    @pl.when(step + 1 < n_steps)
    def _():
        issue(step + 1, (step + 1) % 2)

    slot = step % 2
    pltpu.make_async_copy(buf.at[slot], buf.at[slot], sems.at[slot]).wait()
    sub = lax.broadcasted_iota(jnp.int32, (8, 128), 0)

    def pick(i, carry):
        halves = [[None, None] for _ in range(n_layers)]
        for half in range(2):
            for k in range(8):
                tok = i * 16 + half * 8 + k
                shift = (k + 8 - off_ref[step * n_tok + tok] % 8) % 8
                for l in range(n_layers):
                    moved = pltpu.roll(buf[slot, tok, l].astype(F32), shift, axis=0)
                    halves[l][half] = moved if k == 0 else jnp.where(sub == k, moved, halves[l][half])
        for l in range(n_layers):
            out_ref[l, pl.ds(pl.multiple_of(i * 16, 16), 16), :] = jnp.concatenate(halves[l], axis=0).astype(BF16)
        return carry

    lax.fori_loop(0, n_tok // 16, pick, 0)


def run_fetch(tables, offsets):
    n_layers, _, e_dim = tables.shape
    n_rows = offsets.shape[0]
    n_steps = n_rows // FETCH_TOK
    return pl.pallas_call(
        functools.partial(fetch_body, n_layers, FETCH_TOK, n_steps),
        grid_spec=pltpu.PrefetchScalarGridSpec(
            num_scalar_prefetch=1,
            grid=(n_steps,),
            in_specs=[pl.BlockSpec(memory_space=pl.ANY)],
            out_specs=pl.BlockSpec((n_layers, FETCH_TOK, e_dim), lambda i, off: (0, i, 0)),
            scratch_shapes=[pltpu.VMEM((2, FETCH_TOK, n_layers, 8, e_dim), BF16), pltpu.SemaphoreType.DMA((2,))],
        ),
        out_shape=jax.ShapeDtypeStruct((n_layers, n_rows, e_dim), BF16),
        cost_estimate=pl.CostEstimate(flops=2_000_000_000, bytes_accessed=30_000_000, transcendentals=0),
        compiler_params=pltpu.CompilerParams(dimension_semantics=('arbitrary',)),
        name='fetch_rows',
    )(offsets, tables)


def place_body(group, n_group, idx_bits, n_blocks, tail, starts_ref, keys_ref, *refs):
    rows_refs, out_ref, buf, sems = refs[:n_group], refs[-3], refs[-2], refs[-1]
    first = (n_blocks * 3) // 4
    tail_step = n_blocks - 1 - first
    step = pl.program_id(0)
    block = (step + first) % n_blocks
    slot = step % PLACE_BUFS

    def copy(at, rows):
        where = pl.ds(pl.multiple_of(((at + first) % n_blocks) * OUT_ROWS, OUT_ROWS), rows)
        which = at % PLACE_BUFS
        return pltpu.make_async_copy(buf.at[which, :, pl.ds(0, rows), :], out_ref.at[pl.ds(group * n_group, n_group), where, :], sems.at[which])

    @pl.when((step >= PLACE_BUFS) & (step != tail_step + PLACE_BUFS))
    def _():
        copy(step - PLACE_BUFS, OUT_ROWS).wait()

    @pl.when(step == tail_step + PLACE_BUFS)
    def _():
        copy(step - PLACE_BUFS, tail).wait()

    buf[slot] = jnp.zeros(buf.shape[1:], F32)
    start, end = starts_ref[block], starts_ref[block + 1]
    base = block * OUT_ROWS

    def go(i, carry):
        prev, accs = carry[0], list(carry[1:])
        for u in range(PLACE_UNROLL):
            key = keys_ref[start + i * PLACE_UNROLL + u]
            src = key & ((1 << idx_bits) - 1)
            row_id = key >> idx_bits
            fresh = row_id != prev
            dst = jnp.minimum(row_id - base, OUT_ROWS)
            for g in range(n_group):
                accs[g] = rows_refs[g][pl.ds(src, 1), :] + jnp.where(fresh, 0.0, accs[g])
                buf[slot, g, pl.ds(dst, 1), :] = accs[g]
            prev = row_id
        return (prev, *accs)

    zero = jnp.zeros((1, buf.shape[3]), F32)
    lax.fori_loop(0, (end - start + PLACE_UNROLL - 1) // PLACE_UNROLL, go, (jnp.int32(-1),) + (zero,) * n_group)

    @pl.when(step != tail_step)
    def _():
        copy(step, OUT_ROWS).start()

    @pl.when(step == tail_step)
    def _():
        copy(step, tail).start()

    @pl.when(step == n_blocks - 1)
    def _():
        for at in range(max(0, n_blocks - PLACE_BUFS), n_blocks):
            copy(at, tail if at == tail_step else OUT_ROWS).wait()


def run_place(group, starts, keys, rows_list, d_tables, shape):
    n_group = len(rows_list)
    n_rows, e_dim = rows_list[0].shape
    idx_bits = (n_rows - 1).bit_length()
    n_blocks = pl.cdiv(shape[1], OUT_ROWS)
    tail = shape[1] - (n_blocks - 1) * OUT_ROWS
    args = [starts, keys, *rows_list]
    in_specs = [pl.BlockSpec((n_rows, e_dim), lambda i, s, k: (0, 0)) for _ in rows_list]
    aliases = {}
    if d_tables is not None:
        aliases = {len(args): 0}
        args.append(d_tables)
        in_specs.append(pl.BlockSpec(memory_space=pl.ANY))
    return pl.pallas_call(
        functools.partial(place_body, group, n_group, idx_bits, n_blocks, tail),
        grid_spec=pltpu.PrefetchScalarGridSpec(
            num_scalar_prefetch=2,
            grid=(n_blocks,),
            in_specs=in_specs,
            out_specs=pl.BlockSpec(memory_space=pl.ANY),
            scratch_shapes=[pltpu.VMEM((PLACE_BUFS, n_group, OUT_ROWS + 8, e_dim), F32), pltpu.SemaphoreType.DMA((PLACE_BUFS,))],
        ),
        out_shape=jax.ShapeDtypeStruct(shape, F32),
        input_output_aliases=aliases,
        cost_estimate=pl.CostEstimate(flops=30_000_000_000, bytes_accessed=n_group * 44_000_000, transcendentals=0),
        compiler_params=pltpu.CompilerParams(dimension_semantics=('arbitrary',), vmem_limit_bytes=56 * 2**20),
        name='place_rows',
    )(*args)


def solution(mesh):
    n_emb = mesh.shape['emb']
    tok_spec = P(('dp', 'emb'))
    act_spec = P(('dp', 'emb'), None)
    table_spec = P(None, 'emb', None)
    full_spec = P(None, None, None)
    swap = [(i, (i + 1) % n_emb) for i in range(n_emb)]

    def device_body(tok_ids, resid_in, cot_out, tables, w_up, w_down, w_gate, w_proj):
        n_layers, range_rows, e_dim = tables.shape
        tok_count = tok_ids.shape[0]
        base = lax.axis_index('emb') * range_rows

        own_off = tok_ids - base
        own_mask = (own_off >= 0) & (own_off < range_rows)
        peer_ids = lax.ppermute(tok_ids, 'emb', swap)
        pair_off = jnp.concatenate([own_off, peer_ids - base])
        spread = (jnp.arange(pair_off.shape[0], dtype=jnp.int32) * 32) % range_rows
        offsets = jnp.where((pair_off >= 0) & (pair_off < range_rows), pair_off, spread)
        served = run_fetch(tables, offsets)
        from_peer = lax.ppermute(served[:, tok_count:], 'emb', swap)
        fetched = jnp.where(own_mask[None, :, None], served[:, :tok_count], from_peer)

        all_ids = lax.all_gather(tok_ids, ('dp', 'emb'), axis=0, tiled=True)
        n_all = all_ids.shape[0]
        idx_bits = (n_all - 1).bit_length()
        all_off = all_ids - base
        all_off = jnp.where((all_off >= 0) & (all_off < range_rows), all_off, range_rows)
        keys = jnp.sort((all_off << idx_bits) | jnp.arange(n_all, dtype=jnp.int32))
        n_blocks = pl.cdiv(range_rows, OUT_ROWS)
        pad = jnp.full((PLACE_UNROLL,), range_rows << idx_bits, jnp.int32)
        bounds = jnp.minimum(jnp.arange(n_blocks + 1, dtype=jnp.int32) * OUT_ROWS, range_rows)
        starts = jnp.sum((all_off[None, :] < bounds[:, None]).astype(jnp.int32), axis=1)

        keys = jnp.concatenate([keys, pad])
        keys, starts, fetched = lax.optimization_barrier((keys, starts, fetched))

        resid_out, xs, dg, gp = run_forward(resid_in, fetched, w_up, w_down, w_gate, w_proj)

        cot = cot_out
        rows_list = [None] * n_layers
        for layer in reversed(range(n_layers)):
            if layer + 2 < n_layers:
                cot, rows_list[layer + 2] = lax.optimization_barrier((cot, rows_list[layer + 2]))
            cot, grad_rows = run_backward(layer, cot, xs, fetched, gp, dg, w_up, w_down, w_gate, w_proj)
            if layer == 0:
                grad_rows, rows_list[1] = lax.optimization_barrier((grad_rows, rows_list[1]))
            rows_list[layer] = lax.all_gather(grad_rows, ('dp', 'emb'), axis=0, tiled=True)

        d_tables = None
        per_group = n_layers // 2
        for group in (1, 0):
            d_tables = run_place(group, starts, keys, rows_list[group * per_group:(group + 1) * per_group], d_tables, tables.shape)
        return resid_out, d_tables

    return jax.shard_map(device_body, mesh=mesh, in_specs=(tok_spec, act_spec, act_spec, table_spec, full_spec, full_spec, full_spec, full_spec), out_specs=(act_spec, table_spec), check_vma=False)
```

```python
import functools

import jax
import jax.numpy as jnp
from jax import lax
from jax.experimental import pallas as pl
from jax.experimental.pallas import tpu as pltpu
from jax.sharding import PartitionSpec as P

NORM_EPS = 1e-6
GELU_K = 0.7978845608028654
GELU_A = 0.044715
F_TILE = 256
RING = 8
SLOPE_RING = 4
FWD_CHUNK = 256
BWD_CHUNK = 1024
OUT_ROWS = 1024
PLACE_UNROLL = 8
PLACE_BUFS = 12
FETCH_TOK = 128
F32 = jnp.float32
BF16 = jnp.bfloat16


def gelu_pair(x):
    sq = x * x
    t = jnp.tanh(x * (GELU_K + (GELU_K * GELU_A) * sq))
    cdf = 0.5 + 0.5 * t
    slope = cdf + (0.5 * x) * (1.0 - t * t) * (GELU_K + (3.0 * GELU_K * GELU_A) * sq)
    return x * cdf, slope


def dot_nn(a, b):
    return lax.dot_general(a, b, (((1,), (0,)), ((), ())), preferred_element_type=F32)


def dot_nt(a, b):
    return lax.dot_general(a, b, (((1,), (1,)), ((), ())), preferred_element_type=F32)


def row_chunks(rows, size):
    return [pl.ds(r, min(size, rows)) for r in range(0, rows, size)]


def weight_copy(src, buf, sems, layer, tile, index, by_rows):
    span = pl.ds(pl.multiple_of(tile * F_TILE, F_TILE), F_TILE)
    part = src.at[layer, span, :] if by_rows else src.at[layer, :, span]
    slot = index & (RING - 1)
    return pltpu.make_async_copy(part, buf.at[slot], sems.at[slot])


def forward_body(n_layers, n_tiles, x_ref, e_ref, wu_ref, wd_ref, wg_ref, wp_ref, out_ref, xs_ref, dg_ref, gp_ref, x_s, u_s, h_s, acc_s, wu_s, wd_s, dg_s, wu_sem, wd_sem, dg_sem):
    layer = pl.program_id(0)
    chunks = row_chunks(x_s.shape[0], FWD_CHUNK)
    total = n_layers * n_tiles
    first = layer * n_tiles

    def up_copy(i):
        return weight_copy(wu_ref, wu_s, wu_sem, i // n_tiles, i % n_tiles, i, False)

    def down_copy(i):
        return weight_copy(wd_ref, wd_s, wd_sem, i // n_tiles, i % n_tiles, i, True)

    def slope_copy(i):
        return pltpu.make_async_copy(dg_s.at[i & (SLOPE_RING - 1)], dg_ref.at[i // n_tiles, i % n_tiles], dg_sem.at[i & (SLOPE_RING - 1)])

    def enter(i):
        @pl.when(i + RING - 1 < total)
        def _():
            up_copy(i + RING - 1).start()

        @pl.when(i + RING - 2 < total)
        def _():
            down_copy(i + RING - 2).start()

        @pl.when(i + 1 < total)
        def _():
            up_copy(i + 1).wait()

        down_copy(i).wait()

        @pl.when(i >= SLOPE_RING)
        def _():
            slope_copy(i - SLOPE_RING).wait()

    def up_half(i, r):
        act, slope = gelu_pair(dot_nn(u_s[r, :], wu_s[i & (RING - 1)]))
        dg_s[i & (SLOPE_RING - 1), r, :] = slope
        h_s[r, :] = act.astype(BF16)

    @pl.when(layer == 0)
    def _():
        for i in range(min(RING - 1, total)):
            up_copy(i).start()
            if i < RING - 2:
                down_copy(i).start()
        x_s[...] = x_ref[...]
        up_copy(0).wait()

    enter(first)
    for r in chunks:
        x_bf = x_s[r, :]
        xs_ref[0, r, :] = x_bf
        x_f = x_bf.astype(F32)
        u = (x_f * lax.rsqrt(jnp.mean(x_f * x_f, axis=-1, keepdims=True) + NORM_EPS)).astype(BF16)
        u_s[r, :] = u
        gate_pre = dot_nn(u, wg_ref[0])
        gp_ref[0, r, :] = gate_pre
        gate_act, _ = gelu_pair(gate_pre)
        mixed = (gate_act * e_ref[0, r, :].astype(F32)).astype(BF16)
        acc_s[r, :] = x_f + dot_nn(mixed, wp_ref[0])
        up_half(first, r)
    slope_copy(first).start()

    def tile_step(tile, carry):
        i = first + tile
        enter(i)
        for r in chunks:
            acc_s[r, :] += dot_nn(h_s[r, :], wd_s[(i - 1) & (RING - 1)])
            up_half(i, r)
        slope_copy(i).start()
        return carry

    lax.fori_loop(1, n_tiles, tile_step, 0)
    for r in chunks:
        x_s[r, :] = (acc_s[r, :] + dot_nn(h_s[r, :], wd_s[(first + n_tiles - 1) & (RING - 1)])).astype(BF16)

    @pl.when(layer == n_layers - 1)
    def _():
        out_ref[...] = x_s[...]
        for i in range(max(0, total - SLOPE_RING), total):
            slope_copy(i).wait()


def run_forward(resid_in, fetched, w_up, w_down, w_gate, w_proj):
    n_layers, d_model, ffn = w_up.shape
    rows, e_dim = resid_in.shape[0], w_gate.shape[2]
    n_tiles = ffn // F_TILE
    whole = pl.BlockSpec((rows, d_model), lambda l: (0, 0))
    in_hbm = pl.BlockSpec(memory_space=pl.ANY)
    per_layer = lambda *s: pl.BlockSpec((1,) + s, lambda l: (l, 0, 0))
    return pl.pallas_call(
        functools.partial(forward_body, n_layers, n_tiles),
        grid=(n_layers,),
        in_specs=[whole, per_layer(rows, e_dim), in_hbm, in_hbm, per_layer(d_model, e_dim), per_layer(e_dim, d_model)],
        out_specs=[whole, per_layer(rows, d_model), in_hbm, per_layer(rows, e_dim)],
        out_shape=[
            jax.ShapeDtypeStruct((rows, d_model), BF16),
            jax.ShapeDtypeStruct((n_layers, rows, d_model), BF16),
            jax.ShapeDtypeStruct((n_layers, n_tiles, rows, F_TILE), F32),
            jax.ShapeDtypeStruct((n_layers, rows, e_dim), F32),
        ],
        scratch_shapes=[
            pltpu.VMEM((rows, d_model), BF16),
            pltpu.VMEM((rows, d_model), BF16),
            pltpu.VMEM((rows, F_TILE), BF16),
            pltpu.VMEM((rows, d_model), F32),
            pltpu.VMEM((RING, d_model, F_TILE), BF16),
            pltpu.VMEM((RING, F_TILE, d_model), BF16),
            pltpu.VMEM((SLOPE_RING, rows, F_TILE), F32),
            pltpu.SemaphoreType.DMA((RING,)),
            pltpu.SemaphoreType.DMA((RING,)),
            pltpu.SemaphoreType.DMA((SLOPE_RING,)),
        ],
        cost_estimate=pl.CostEstimate(flops=4 * n_layers * rows * d_model * ffn, bytes_accessed=n_layers * 40_000_000, transcendentals=0),
        compiler_params=pltpu.CompilerParams(dimension_semantics=('arbitrary',), vmem_limit_bytes=56 * 2**20),
        name='forward',
    )(resid_in, fetched, w_up, w_down, w_gate, w_proj)


def backward_body(layer, n_tiles, c_ref, xs_ref, e_ref, gp_ref, dg_ref, wu_ref, wd_ref, wg_ref, wp_ref, cot_ref, gr_ref, xs_s, dng_s, du_s, acc_s, wu_s, wd_s, dg_s, wu_sem, wd_sem, dg_sem, xs_sem):
    chunks = row_chunks(c_ref.shape[0], BWD_CHUNK)

    def up_copy(i):
        return weight_copy(wu_ref, wu_s, wu_sem, layer, i, i, False)

    def down_copy(i):
        return weight_copy(wd_ref, wd_s, wd_sem, layer, i, i, True)

    def slope_copy(i):
        return pltpu.make_async_copy(dg_ref.at[layer, i], dg_s.at[i & (RING - 1)], dg_sem.at[i & (RING - 1)])

    saved_copy = pltpu.make_async_copy(xs_ref.at[layer], xs_s, xs_sem)

    def enter(i):
        @pl.when(i + RING - 1 < n_tiles)
        def _():
            down_copy(i + RING - 1).start()
            slope_copy(i + RING - 1).start()

        @pl.when(i + RING - 2 < n_tiles)
        def _():
            up_copy(i + RING - 2).start()

        @pl.when(i + 1 < n_tiles)
        def _():
            down_copy(i + 1).wait()
            slope_copy(i + 1).wait()

        up_copy(i).wait()

    def hidden_half(i, r):
        d_hidden = dot_nt(c_ref[r, :], wd_s[i & (RING - 1)]).astype(BF16).astype(F32)
        du_s[r, :] = (d_hidden * dg_s[i & (RING - 1), r, :]).astype(BF16)

    for i in range(min(RING - 1, n_tiles)):
        down_copy(i).start()
        slope_copy(i).start()
        if i < RING - 2:
            up_copy(i).start()
    saved_copy.start()
    down_copy(0).wait()
    slope_copy(0).wait()
    enter(0)
    for r in chunks:
        d_mixed = dot_nt(c_ref[r, :], wp_ref[0]).astype(BF16).astype(F32)
        gate_act, slope = gelu_pair(gp_ref[0, r, :])
        gr_ref[r, :] = gate_act * d_mixed
        d_gate = (slope * (d_mixed * e_ref[0, r, :].astype(F32))).astype(BF16)
        dng_s[r, :] = dot_nt(d_gate, wg_ref[0]).astype(BF16)
        acc_s[r, :] = jnp.zeros((r.size, acc_s.shape[1]), F32)
        hidden_half(0, r)

    def tile_step(i, carry):
        enter(i)
        for r in chunks:
            acc_s[r, :] += dot_nt(du_s[r, :], wu_s[(i - 1) & (RING - 1)])
            hidden_half(i, r)
        return carry

    lax.fori_loop(1, n_tiles, tile_step, 0)
    saved_copy.wait()
    for r in row_chunks(c_ref.shape[0], FWD_CHUNK):
        acc = acc_s[r, :] + dot_nt(du_s[r, :], wu_s[(n_tiles - 1) % RING])
        d_n = (acc.astype(BF16).astype(F32) + dng_s[r, :].astype(F32)).astype(BF16).astype(F32)
        x_f = xs_s[r, :].astype(F32)
        inv = lax.rsqrt(jnp.mean(x_f * x_f, axis=-1, keepdims=True) + NORM_EPS)
        proj = jnp.mean(d_n * x_f, axis=-1, keepdims=True)
        d_x = d_n * inv - x_f * (inv * inv * inv * proj)
        cot_ref[r, :] = (c_ref[r, :].astype(F32) + d_x).astype(BF16)


def run_backward(layer, cot, xs, fetched, gp, dg, w_up, w_down, w_gate, w_proj):
    _, d_model, ffn = w_up.shape
    rows, e_dim = cot.shape[0], w_gate.shape[2]
    n_tiles = ffn // F_TILE
    whole = lambda *s: pl.BlockSpec(s, lambda j: (0, 0))
    in_hbm = pl.BlockSpec(memory_space=pl.ANY)
    at_layer = lambda *s: pl.BlockSpec((1,) + s, lambda j: (layer, 0, 0))
    return pl.pallas_call(
        functools.partial(backward_body, layer, n_tiles),
        grid=(1,),
        in_specs=[whole(rows, d_model), in_hbm, at_layer(rows, e_dim), at_layer(rows, e_dim), in_hbm, in_hbm, in_hbm, at_layer(d_model, e_dim), at_layer(e_dim, d_model)],
        out_specs=[whole(rows, d_model), whole(rows, e_dim)],
        out_shape=[jax.ShapeDtypeStruct((rows, d_model), BF16), jax.ShapeDtypeStruct((rows, e_dim), F32)],
        scratch_shapes=[
            pltpu.VMEM((rows, d_model), BF16),
            pltpu.VMEM((rows, d_model), BF16),
            pltpu.VMEM((rows, F_TILE), BF16),
            pltpu.VMEM((rows, d_model), F32),
            pltpu.VMEM((RING, d_model, F_TILE), BF16),
            pltpu.VMEM((RING, F_TILE, d_model), BF16),
            pltpu.VMEM((RING, rows, F_TILE), F32),
            pltpu.SemaphoreType.DMA((RING,)),
            pltpu.SemaphoreType.DMA((RING,)),
            pltpu.SemaphoreType.DMA((RING,)),
            pltpu.SemaphoreType.DMA,
        ],
        cost_estimate=pl.CostEstimate(flops=4 * rows * d_model * ffn, bytes_accessed=40_000_000, transcendentals=0),
        compiler_params=pltpu.CompilerParams(dimension_semantics=('arbitrary',), vmem_limit_bytes=56 * 2**20),
        name='backward',
    )(cot, xs, fetched, gp, dg, w_up, w_down, w_gate, w_proj)


def fetch_body(n_layers, n_tok, n_steps, off_ref, table_ref, out_ref, buf, sems):
    step = pl.program_id(0)

    def issue(at, slot):
        def go(i, carry):
            for k in range(8):
                tok = i * 8 + k
                tile = off_ref[at * n_tok + tok] >> 3
                pltpu.make_async_copy(table_ref.at[:, pl.ds(pl.multiple_of(tile * 8, 8), 8), :], buf.at[slot, tok], sems.at[slot]).start(priority=k % 2)
            return carry

        lax.fori_loop(0, n_tok // 8, go, 0)

    @pl.when(step == 0)
    def _():
        issue(0, 0)

    @pl.when(step + 1 < n_steps)
    def _():
        issue(step + 1, (step + 1) % 2)

    slot = step % 2
    pltpu.make_async_copy(buf.at[slot], buf.at[slot], sems.at[slot]).wait()
    sub = lax.broadcasted_iota(jnp.int32, (8, 128), 0)

    def pick(i, carry):
        halves = [[None, None] for _ in range(n_layers)]
        for half in range(2):
            for k in range(8):
                tok = i * 16 + half * 8 + k
                shift = (k - off_ref[step * n_tok + tok]) & 7
                for l in range(n_layers):
                    moved = pltpu.roll(buf[slot, tok, l].astype(F32), shift, axis=0)
                    halves[l][half] = moved if k == 0 else jnp.where(sub == k, moved, halves[l][half])
        for l in range(n_layers):
            out_ref[l, pl.ds(pl.multiple_of(i * 16, 16), 16), :] = jnp.concatenate(halves[l], axis=0).astype(BF16)
        return carry

    lax.fori_loop(0, n_tok // 16, pick, 0)


def run_fetch(tables, offsets):
    n_layers, _, e_dim = tables.shape
    n_rows = offsets.shape[0]
    n_steps = n_rows // FETCH_TOK
    return pl.pallas_call(
        functools.partial(fetch_body, n_layers, FETCH_TOK, n_steps),
        grid_spec=pltpu.PrefetchScalarGridSpec(
            num_scalar_prefetch=1,
            grid=(n_steps,),
            in_specs=[pl.BlockSpec(memory_space=pl.ANY)],
            out_specs=pl.BlockSpec((n_layers, FETCH_TOK, e_dim), lambda i, off: (0, i, 0)),
            scratch_shapes=[pltpu.VMEM((2, FETCH_TOK, n_layers, 8, e_dim), BF16), pltpu.SemaphoreType.DMA((2,))],
        ),
        out_shape=jax.ShapeDtypeStruct((n_layers, n_rows, e_dim), BF16),
        cost_estimate=pl.CostEstimate(flops=2_000_000_000, bytes_accessed=30_000_000, transcendentals=0),
        compiler_params=pltpu.CompilerParams(dimension_semantics=('arbitrary',)),
        name='fetch_rows',
    )(offsets, tables)


def place_body(group, n_group, idx_bits, n_blocks, tail, starts_ref, keys_ref, *refs):
    rows_refs, out_ref, buf, sems = refs[:n_group], refs[-3], refs[-2], refs[-1]
    first = (n_blocks * 3) // 4
    tail_step = n_blocks - 1 - first
    step = pl.program_id(0)
    block = (step + first) % n_blocks
    slot = step % PLACE_BUFS

    def copy(at, rows):
        where = pl.ds(pl.multiple_of(((at + first) % n_blocks) * OUT_ROWS, OUT_ROWS), rows)
        which = at % PLACE_BUFS
        return pltpu.make_async_copy(buf.at[which, :, pl.ds(0, rows), :], out_ref.at[pl.ds(group * n_group, n_group), where, :], sems.at[which])

    @pl.when((step >= PLACE_BUFS) & (step != tail_step + PLACE_BUFS))
    def _():
        copy(step - PLACE_BUFS, OUT_ROWS).wait()

    @pl.when(step == tail_step + PLACE_BUFS)
    def _():
        copy(step - PLACE_BUFS, tail).wait()

    buf[slot] = jnp.zeros(buf.shape[1:], F32)
    start, end = starts_ref[block], starts_ref[block + 1]
    base = block * OUT_ROWS

    def go(i, carry):
        prev, accs = carry[0], list(carry[1:])
        for u in range(PLACE_UNROLL):
            key = keys_ref[start + i * PLACE_UNROLL + u]
            src = key & ((1 << idx_bits) - 1)
            row_id = key >> idx_bits
            fresh = row_id != prev
            dst = jnp.minimum(row_id - base, OUT_ROWS)
            for g in range(n_group):
                accs[g] = rows_refs[g][pl.ds(src, 1), :] + jnp.where(fresh, 0.0, accs[g])
                buf[slot, g, pl.ds(dst, 1), :] = accs[g]
            prev = row_id
        return (prev, *accs)

    zero = jnp.zeros((1, buf.shape[3]), F32)
    lax.fori_loop(0, (end - start + PLACE_UNROLL - 1) // PLACE_UNROLL, go, (jnp.int32(-1),) + (zero,) * n_group)

    @pl.when(step != tail_step)
    def _():
        copy(step, OUT_ROWS).start()

    @pl.when(step == tail_step)
    def _():
        copy(step, tail).start()

    @pl.when(step == n_blocks - 1)
    def _():
        for at in range(max(0, n_blocks - PLACE_BUFS), n_blocks):
            copy(at, tail if at == tail_step else OUT_ROWS).wait()


def run_place(group, starts, keys, rows_list, d_tables, shape):
    n_group = len(rows_list)
    n_rows, e_dim = rows_list[0].shape
    idx_bits = (n_rows - 1).bit_length()
    n_blocks = pl.cdiv(shape[1], OUT_ROWS)
    tail = shape[1] - (n_blocks - 1) * OUT_ROWS
    args = [starts, keys, *rows_list]
    in_specs = [pl.BlockSpec((n_rows, e_dim), lambda i, s, k: (0, 0)) for _ in rows_list]
    aliases = {}
    if d_tables is not None:
        aliases = {len(args): 0}
        args.append(d_tables)
        in_specs.append(pl.BlockSpec(memory_space=pl.ANY))
    return pl.pallas_call(
        functools.partial(place_body, group, n_group, idx_bits, n_blocks, tail),
        grid_spec=pltpu.PrefetchScalarGridSpec(
            num_scalar_prefetch=2,
            grid=(n_blocks,),
            in_specs=in_specs,
            out_specs=pl.BlockSpec(memory_space=pl.ANY),
            scratch_shapes=[pltpu.VMEM((PLACE_BUFS, n_group, OUT_ROWS + 8, e_dim), F32), pltpu.SemaphoreType.DMA((PLACE_BUFS,))],
        ),
        out_shape=jax.ShapeDtypeStruct(shape, F32),
        input_output_aliases=aliases,
        cost_estimate=pl.CostEstimate(flops=30_000_000_000, bytes_accessed=n_group * 44_000_000, transcendentals=0),
        compiler_params=pltpu.CompilerParams(dimension_semantics=('arbitrary',), vmem_limit_bytes=56 * 2**20),
        name='place_rows',
    )(*args)


def solution(mesh):
    n_emb, n_dp = mesh.shape['emb'], mesh.shape['dp']
    tok_spec = P(('dp', 'emb'))
    act_spec = P(('dp', 'emb'), None)
    table_spec = P(None, 'emb', None)
    full_spec = P(None, None, None)
    swap = [(i, (i + 1) % n_emb) for i in range(n_emb)]

    def device_body(tok_ids, resid_in, cot_out, tables, w_up, w_down, w_gate, w_proj):
        n_layers, range_rows, e_dim = tables.shape
        tok_count = tok_ids.shape[0]
        base = lax.axis_index('emb') * range_rows

        own_off = tok_ids - base
        own_mask = (own_off >= 0) & (own_off < range_rows)
        peer_ids = lax.ppermute(tok_ids, 'emb', swap)
        pair_off = jnp.concatenate([own_off, peer_ids - base])
        spread = (jnp.arange(pair_off.shape[0], dtype=jnp.int32) * 32) % range_rows
        offsets = jnp.where((pair_off >= 0) & (pair_off < range_rows), pair_off, spread)
        served = run_fetch(tables, offsets)
        from_peer = lax.ppermute(served[:, tok_count:], 'emb', swap)
        fetched = jnp.where(own_mask[None, :, None], served[:, :tok_count], from_peer)

        all_ids = jnp.concatenate([tok_ids, peer_ids])
        dp_at = lax.axis_index('dp')
        emb_at = lax.axis_index('emb')
        owners = dp_at * n_emb + jnp.array([0, 1]) * (1 - 2 * emb_at) + emb_at
        for step in (1, 2):
            hop = [(i, i ^ step) for i in range(n_dp)]
            all_ids = jnp.concatenate([all_ids, lax.ppermute(all_ids, 'dp', hop)])
        owners = jnp.concatenate([owners + ((dp_at ^ far) - dp_at) * n_emb for far in range(n_dp)])
        n_all = all_ids.shape[0]
        idx_bits = (n_all - 1).bit_length()
        token_at = (owners[:, None] * tok_count + jnp.arange(tok_count, dtype=jnp.int32)[None, :]).reshape(-1).astype(jnp.int32)
        all_off = all_ids - base
        all_off = jnp.where((all_off >= 0) & (all_off < range_rows), all_off, range_rows)
        keys = jnp.sort((all_off << idx_bits) | token_at)
        n_blocks = pl.cdiv(range_rows, OUT_ROWS)
        pad = jnp.full((PLACE_UNROLL,), range_rows << idx_bits, jnp.int32)
        bounds = jnp.minimum(jnp.arange(n_blocks + 1, dtype=jnp.int32) * OUT_ROWS, range_rows)
        starts = jnp.sum((all_off[None, :] < bounds[:, None]).astype(jnp.int32), axis=1)

        keys = jnp.concatenate([keys, pad])
        keys, starts, fetched = lax.optimization_barrier((keys, starts, fetched))

        resid_out, xs, dg, gp = run_forward(resid_in, fetched, w_up, w_down, w_gate, w_proj)

        cot = cot_out
        rows_list = [None] * n_layers
        for layer in reversed(range(n_layers)):
            if layer + 2 < n_layers:
                cot, rows_list[layer + 2] = lax.optimization_barrier((cot, rows_list[layer + 2]))
            cot, grad_rows = run_backward(layer, cot, xs, fetched, gp, dg, w_up, w_down, w_gate, w_proj)
            if layer == 0:
                grad_rows, rows_list[1] = lax.optimization_barrier((grad_rows, rows_list[1]))
            rows_list[layer] = lax.all_gather(grad_rows, ('dp', 'emb'), axis=0, tiled=True)

        d_tables = None
        per_group = n_layers // 2
        for group in (1, 0):
            d_tables = run_place(group, starts, keys, rows_list[group * per_group:(group + 1) * per_group], d_tables, tables.shape)
        return resid_out, d_tables

    return jax.shard_map(device_body, mesh=mesh, in_specs=(tok_spec, act_spec, act_spec, table_spec, full_spec, full_spec, full_spec, full_spec), out_specs=(act_spec, table_spec), check_vma=False)
```
